32 devices in a mesh: lam: 16 (over z, x, core), atom: 2 (over y).
Axes of the slice: x: 2, y: 2, z: 4, core: 2. Of those that a mesh axis runs over, the one named last changes fastest.
Arguments:
- coords: float32 [16, 3, 16384], P('lam', None, 'atom'), may hold values from 0 to 1
- velocities: float32 [16, 3, 16384], P('lam', None, 'atom'), may hold values from -6 to 6
- coupling: float32 [16, 2, 16384], P('lam', None, 'atom'), may hold values from 0.2 to 1
- charges: float32 [16384], replicated, may hold values from -1.5 to 1.5
- types: int32 [16384], replicated, may hold values from 0 to 15
- type_sigma: float32 [16], replicated, may hold values from 0.25 to 0.4
- type_eps: float32 [16], replicated, may hold values from 0.1 to 1
- near_tiles: int32 [128, 5], P('atom'), may hold values from 0 to 127
- accept: int32 [16], replicated, may hold values from 0 to 1, as said below
Outputs:
- energies: float32 [16, 3], P('lam')
- forces: float32 [16, 3, 16384], P('lam', None, 'atom')
- new_coords: float32 [16, 3, 16384], P('lam', None, 'atom')
- new_velocities: float32 [16, 3, 16384], P('lam', None, 'atom')
The draws below stay inside these ranges and needn't reach their ends.
Inputs may be any that keep to these rules, and one draw needn't show every extreme that they name: accept[r] = 1 exchanges replicas r and r + 1 (modulo 16); no two consecutive entries around the cycle are both 1.
All inputs are finite; a program needn't handle non-finite values.
Results may differ from the reference program's by a relative error of at most 0.0003.
Values sent between devices are 32-bit elements; how exact they have to be, the bound alone decides.
A program may use at most 64 MiB of HBM per device.

```python
import math
from functools import partial
import jax
import jax.numpy as jnp
from jax import lax

TILE = 128
NEAR = 5
NTYPES = 16
REPLICAS = 16
ATOMS = 16384
TILES = 128


def draw_accept(key, part):
    coins = jax.random.randint(jax.random.fold_in(key, 11), (REPLICAS,), 0, 2)
    return (coins * (1 - jnp.roll(coins, 1))).astype(jnp.int32)


def touch_ends(drawn, own_key, smallest, high):
    extent = drawn.shape
    spot = [jax.random.randint(jax.random.fold_in(own_key, axis), (), 0, extent[axis]) for axis in range(len(extent))]
    drawn = drawn.at[tuple(spot)].set(smallest)
    longest = extent.index(max(extent))
    spot[longest] = (spot[longest] + 1) % extent[longest]
    return drawn.at[tuple(spot)].set(high)


def block_levels(key, dims, shards, low, high):
    level = 1.0
    for position, blocks in shards:
        steps = jax.random.uniform(jax.random.fold_in(jax.random.fold_in(key, 6), position), (blocks,), jnp.float32, low / len(shards), high / len(shards))
        level = level * jnp.repeat(jnp.exp(steps), dims[position] // blocks).reshape((-1,) + (1,) * (len(dims) - 1 - position))
    return level


def centred(stream_key, shape, scale, bound, split=(), held_as=jnp.bfloat16):
    factor_of = block_levels(stream_key, shape, split, -0.22, 0.18) if split else 1.0
    array = jax.random.normal(stream_key, shape, jnp.float32) * scale * factor_of
    return jnp.minimum(jnp.maximum(array, -bound), bound).astype(held_as)


def setup_inputs(seed: int = 0) -> dict:
    streams_of = jax.random.split(jax.random.key(seed), 10)
    coords = jnp.clip(1.0 * jax.random.uniform(streams_of[0], (REPLICAS, 3, ATOMS), jnp.float32) ** block_levels(streams_of[0], (REPLICAS, 3, ATOMS), ((0, 16), (2, 2)), -0.2, 0.2), 0.0, 1.0)
    velocities = centred(streams_of[1], (REPLICAS, 3, ATOMS), 1.0, 6.0, ((0, 16), (2, 2)), jnp.float32)
    coupling = jnp.clip(jnp.exp(math.log(1.0) - 1.609438 * jax.random.uniform(streams_of[2], (REPLICAS, 2, ATOMS), jnp.float32) ** block_levels(streams_of[2], (REPLICAS, 2, ATOMS), ((0, 16), (2, 2)), -0.2, 0.2)), 0.2, 1.0)
    charges = centred(streams_of[3], (ATOMS,), 0.3, 1.5, (), jnp.float32)
    types = touch_ends(jax.random.randint(streams_of[4], (ATOMS,), 0, NTYPES), jax.random.fold_in(streams_of[4], 1), 0, NTYPES - 1).astype(jnp.int32)
    type_sigma = jnp.clip(jnp.exp(jax.random.uniform(streams_of[5], (NTYPES,), jnp.float32, math.log(0.25), math.log(0.4))), 0.25, 0.4)
    type_eps = jnp.clip(jnp.exp(jax.random.uniform(streams_of[6], (NTYPES,), jnp.float32, math.log(0.1), math.log(1.0))), 0.1, 1.0)
    near_tiles = touch_ends(jax.random.randint(streams_of[7], (TILES, NEAR), 0, TILES), jax.random.fold_in(streams_of[7], 1), 0, TILES - 1).astype(jnp.int32)
    accept = draw_accept(jax.random.fold_in(streams_of[9], 71), 0)
    return dict(coords=coords, velocities=velocities, coupling=coupling, charges=charges, types=types, type_sigma=type_sigma, type_eps=type_eps, near_tiles=near_tiles, accept=accept)


DELTA_SOFT = 0.05

def atom_params(charges, types, type_sigma, type_eps, coupling_whole):
    levels = lax.broadcasted_iota(jnp.int32, (type_sigma.shape[0], types.shape[0]), 0)
    onehot = (levels == types[None, :]).astype(jnp.float32)
    table = jnp.stack([type_sigma, jnp.sqrt(type_eps)])
    looked = jnp.dot(table, onehot, precision=lax.Precision.HIGHEST)
    return jnp.stack([charges * coupling_whole[0], looked[1] * coupling_whole[1], looked[0]])

def pair_block(inputs, with_force):
    rows_pos, cols_pos, rows_par, cols_par, rows_idx, cols_idx = inputs
    delta = rows_pos[:, :, None, :, None] - cols_pos[:, :, :, None, :]
    squared = lax.optimization_barrier(jnp.sum(delta * delta, axis=0))
    charge_pair = rows_par[0][:, None, :, None] * cols_par[0][:, :, None, :]
    depth_pair = rows_par[1][:, None, :, None] * cols_par[1][:, :, None, :]
    sigma_pair = 0.5 * (rows_par[2][:, None, :, None] + cols_par[2][:, :, None, :])
    sigma_area = sigma_pair * sigma_pair
    pair_keep = (rows_idx[:, None, :, None] != cols_idx[:, :, None, :]).astype(jnp.float32)
    inverse = lax.rsqrt(squared + DELTA_SOFT)
    ratio = sigma_area / (squared + sigma_area)
    cubed = ratio * ratio * ratio
    energy_pair = charge_pair * inverse + 4.0 * depth_pair * (cubed * cubed - cubed)
    total = jnp.sum(energy_pair * pair_keep)
    if not with_force:
        return (total, jnp.zeros_like(rows_pos))
    slope = -0.5 * charge_pair * inverse * inverse * inverse - 4.0 * depth_pair * (6.0 * cubed * ratio * ratio - 3.0 * ratio * ratio) * ratio * ratio / sigma_area
    weight = -2.0 * slope * pair_keep
    force = lax.optimization_barrier(jnp.sum(weight[None] * delta, axis=(2, 4)))
    return (total, force)

def evaluate(own_rows, whole, params, first_row, tile_list, with_force):
    count = own_rows.shape[1]
    row_tiles = count // TILE
    group = math.gcd(row_tiles, 4)
    blocks = row_tiles // group
    listed = tile_list.shape[1]
    rows_pos = own_rows.reshape(3, blocks, group, TILE).transpose(1, 0, 2, 3)
    own_par = lax.dynamic_slice_in_dim(params, first_row, count, 1)
    rows_par = own_par.reshape(3, blocks, group, TILE).transpose(1, 0, 2, 3)
    cols_pos = whole.reshape(3, -1, TILE)[:, tile_list].reshape(3, blocks, group, listed, TILE).transpose(1, 0, 2, 3, 4)
    cols_par = params.reshape(3, -1, TILE)[:, tile_list].reshape(3, blocks, group, listed, TILE).transpose(1, 0, 2, 3, 4)
    rows_idx = (first_row + jnp.arange(count, dtype=jnp.int32)).reshape(blocks, group, TILE)
    cols_idx = (tile_list[:, :, None] * TILE + jnp.arange(TILE, dtype=jnp.int32)[None, None, :]).reshape(blocks, group, listed, TILE)
    totals, forces = lax.map(partial(pair_block, with_force=with_force), (rows_pos, cols_pos, rows_par, cols_par, rows_idx, cols_idx))
    return (jnp.sum(totals), forces.transpose(1, 0, 2, 3).reshape(3, count))

def reference(coords, velocities, coupling, charges, types, type_sigma, type_eps, near_tiles, accept):
    count = coords.shape[0]

    def replica_terms(index):
        params = atom_params(charges, types, type_sigma, type_eps, coupling[index])
        own_coords = coords[index]
        lower_coords = coords[(index + count - 1) % count]
        upper_coords = coords[(index + 1) % count]
        energy_own, force = evaluate(own_coords, own_coords, params, 0, near_tiles, True)
        energy_low, unused = evaluate(lower_coords, lower_coords, params, 0, near_tiles, False)
        energy_up, unused = evaluate(upper_coords, upper_coords, params, 0, near_tiles, False)
        return (jnp.stack([energy_own, energy_low, energy_up]), force)
    totals_all, forces = lax.map(replica_terms, jnp.arange(count, dtype=jnp.int32))
    scale = 0.5 / ATOMS
    energies = jnp.stack([totals_all[:, 0], jnp.roll(totals_all[:, 2], 1), jnp.roll(totals_all[:, 1], -1)], axis=1) * scale
    upper_flag = (accept == 1)[:, None, None]
    lower_flag = (jnp.roll(accept, 1) == 1)[:, None, None]
    new_coords = jnp.where(upper_flag, jnp.roll(coords, -1, axis=0), jnp.where(lower_flag, jnp.roll(coords, 1, axis=0), coords))
    new_velocities = jnp.where(upper_flag, jnp.roll(velocities, -1, axis=0), jnp.where(lower_flag, jnp.roll(velocities, 1, axis=0), velocities))
    return (energies, forces, new_coords, new_velocities)
```

```python
from functools import partial

import jax
import jax.numpy as jnp
from jax import lax
from jax.experimental import pallas as pl
from jax.experimental.pallas import tpu as pltpu
from jax.sharding import PartitionSpec as P

TILE = 128
DELTA_SOFT = 0.05
SUB = 16
DEPTH = 32
COLS = 2
UNROLL = 2
GROUP = 8


def moved(x, lam_by, atom_by):
    cycle, parts = lax.axis_size("lam"), lax.axis_size("atom")
    pairs = []
    for r in range(cycle):
        for a in range(parts):
            source = ((r - lam_by) % cycle) * parts + (a + atom_by) % parts
            pairs.append((source, r * parts + a))
    return lax.ppermute(x, ("lam", "atom"), pairs)


def halved(x):
    high = x.astype(jnp.bfloat16)
    low = x - high.astype(jnp.float32)
    return jnp.concatenate([high, low.astype(jnp.bfloat16)], axis=1)


def rounded(x):
    return x.astype(jnp.bfloat16).astype(jnp.float32)


def tiles_kernel(parts, listed, *refs):
    where_ref, near_ref, sigma_ref, eps_ref, charges_ref, types_ref = refs[:6]
    halves = refs[6 : 6 + 3 * parts]
    rest = refs[6 + 3 * parts :]
    force_ref, energy_ref, cols, near_feat, own_feat, lhs_e, lhs_f = rest[:7]
    geos = rest[7 : 7 + UNROLL]
    sums = rest[7 + UNROLL : 7 + 2 * UNROLL]
    width = halves[0].shape[2]
    atoms = cols.shape[1]
    row_tiles = width // TILE
    part = where_ref[0]
    first_tile = part * row_tiles

    kinds = types_ref[...]
    radius = jnp.zeros(kinds.shape, jnp.float32)
    depth = jnp.zeros(kinds.shape, jnp.float32)
    for level in range(sigma_ref.shape[0]):
        here = kinds == level
        radius = jnp.where(here, sigma_ref[level], radius)
        depth = jnp.where(here, eps_ref[level], depth)
    cols[3:4, :] = 0.5 * radius
    cols[4:8, :] = jnp.zeros((4, atoms), jnp.float32)
    cols[11:12, :] = jnp.zeros((1, atoms), jnp.float32)
    cols[15:16, :] = jnp.zeros((1, atoms), jnp.float32)
    base = 2.0 * jnp.sqrt(depth)
    spans = []
    for step in range(parts):
        start = pl.multiple_of(lax.rem(part + step, parts) * width, TILE)
        spans.append(pl.ds(start, width))
        cols[0:3, spans[step]] = halves[step][0, 0:3] - 0.5
    for h in range(3):
        for step in range(parts):
            block = halves[parts * h + step]
            last = block.shape[1]
            cols[8 + h : 9 + h, spans[step]] = block[0, last - 2 : last - 1]
            cols[12 + h : 13 + h, spans[step]] = block[0, last - 1 : last]
        cols[8 + h : 9 + h, :] = cols[8 + h : 9 + h, :] * charges_ref[...]
        cols[12 + h : 13 + h, :] = cols[12 + h : 13 + h, :] * base

    def rows_of(n):
        return lax.broadcasted_iota(jnp.int32, (8, n), 0)

    def base_rows(span):
        four = cols[0:4, span]
        return jnp.concatenate([four, four], axis=0)

    def thirds(x):
        high = rounded(x)
        low = x - high
        mid = rounded(low)
        return high, mid, low - mid

    def near_part(c):
        span = pl.ds(pl.multiple_of(c * TILE, TILE), TILE)
        sub = rows_of(TILE)
        quad = sub % 4
        f8 = base_rows(span)
        high, mid, low = thirds(f8)
        sign = jnp.where(quad == 3, 2.0, -2.0).astype(jnp.float32)
        square = f8 * f8
        norm = square[0:1] + square[1:2] + square[2:3]
        mixed = jnp.where(sub < 3, norm, square[3:4])
        nh, nm, nl = thirds(mixed)
        last = jnp.where(quad == 0, nh, jnp.where(quad == 1, nm, nl))
        last = jnp.where(sub == 3, nh, jnp.where(sub == 4, nm, last))
        last = jnp.where(sub >= 5, 1.0, last)
        feats = jnp.concatenate([high * sign, mid * sign, jnp.where(sub < 4, high, low) * sign, last], axis=0)
        near_feat[span, :] = feats.T.astype(jnp.bfloat16)
        own8 = cols[8:16, span]
        oh = rounded(own8)
        lhs_e[:, span] = jnp.concatenate([oh, own8 - oh], axis=0).astype(jnp.bfloat16)
        pos = jnp.where(quad == 3, 1.0, f8)
        scale = jnp.where(sub < 4, own8[0:1], 6.0 * own8[4:5])
        wide = pos * scale
        wh = rounded(wide)
        lhs_f[:, span] = jnp.concatenate([wh, wide - wh], axis=0).astype(jnp.bfloat16)

    def near_parts(c, carry):
        for i in range(GROUP):
            near_part(GROUP * c + i)
        return carry

    lax.fori_loop(0, atoms // (GROUP * TILE), near_parts, 0)

    def own_part(c, carry):
        span = pl.ds(pl.multiple_of((first_tile + c) * TILE, TILE), TILE)
        sub = rows_of(TILE)
        quad = sub % 4
        f8 = base_rows(span)
        high, mid, low = thirds(f8)
        square = f8 * f8
        norm = square[0:1] + square[1:2] + square[2:3]
        first = jnp.where(sub < 4, high, mid)
        third = jnp.where(sub < 4, low, high)
        outs = []
        for which in range(COLS):
            const = (norm + DELTA_SOFT, norm + square[3:4], square[3:4])[which]
            ch, cm, cl = thirds(const)
            ones = sub < (3, 5, 5)[which]
            if which == 2:
                ones = (sub == 3) | (sub == 4)
            last = jnp.where(ones, 1.0, 0.0)
            last = jnp.where(sub == 5, ch, jnp.where(sub == 6, cm, jnp.where(sub == 7, cl, last)))
            keep = (quad != 3, quad <= 3, quad == 3)[which]
            a = jnp.where(keep, first, 0.0)
            outs.append(jnp.concatenate([a, a, jnp.where(keep, third, 0.0), last], axis=0))
        place = pl.ds(pl.multiple_of(c * (COLS * TILE), TILE), COLS * TILE)
        own_feat[:, place] = jnp.concatenate(outs, axis=1).astype(jnp.bfloat16)
        return carry

    lax.fori_loop(0, row_tiles, own_part, 0)

    def geometry(t, s):
        place = pl.ds(pl.multiple_of(t * (COLS * TILE), TILE), COLS * TILE)
        rhs = own_feat[:, place]
        for k in range(listed):
            span = pl.ds(pl.multiple_of(near_ref[t, k] * TILE, TILE), TILE)
            geos[s][k] = jnp.dot(near_feat[span, :], rhs, preferred_element_type=jnp.float32)

    def blocks(t, s):
        total = None
        for k in range(listed):
            span = pl.ds(pl.multiple_of(near_ref[t, k] * TILE, TILE), TILE)
            invs, charge, ljs, well = [], [], [], []
            for b in range(TILE // SUB):
                rows = pl.ds(b * SUB, SUB)
                inv = lax.rsqrt(geos[s][k, rows, 0:TILE])
                charge.append(halved(inv * (inv * inv)))
                invs.append(inv.astype(jnp.bfloat16))
            for b in range(TILE // SUB):
                rows = pl.ds(b * SUB, SUB)
                both = geos[s][k, rows, TILE : 2 * TILE]
                root = lax.rsqrt(both)
                p = root * root
                if COLS == 3:
                    x = geos[s][k, rows, 2 * TILE : 3 * TILE] * p
                else:
                    x = ((both - geos[s][k, rows, 0:TILE]) + DELTA_SOFT) * p
                x3 = x * x * x
                low = x3 - 1.0
                ljs.append((x3 * low).astype(jnp.bfloat16))
                well.append(halved((x3 * p) * (x3 + low)))
            le = lhs_e[:, span]
            lf = lhs_f[:, span]
            fc = jnp.dot(lf, jnp.concatenate(charge, axis=0), preferred_element_type=jnp.float32)
            fw = jnp.dot(lf, jnp.concatenate(well, axis=0), preferred_element_type=jnp.float32)
            pairs = jnp.concatenate([jnp.concatenate(invs, axis=0), jnp.concatenate(ljs, axis=0)], axis=1)
            en = jnp.dot(le, pairs, preferred_element_type=jnp.float32)
            new = (fc, fw, en)
            total = new if total is None else tuple(x + y for x, y in zip(total, new))
        for i, x in enumerate(total):
            sums[s][i] = x

    def finish(t, s, carry):
        totals, selfs = carry
        own = first_tile + t
        own_span = pl.ds(pl.multiple_of(own * TILE, TILE), TILE)
        out_span = pl.ds(pl.multiple_of(t * TILE, TILE), TILE)
        sub = rows_of(TILE)
        quad = sub % 4
        mine = cols[8:16, own_span]
        fold = []
        for i in range(2):
            x = sums[s][i, 0:8] + sums[s][i, 8:16]
            fold.append(x[:, :TILE] + x[:, TILE:])
        en = sums[s][2, 0:8] + sums[s][2, 8:16]
        totals = totals + mine * jnp.where(sub < 4, en[:, :TILE], en[:, TILE:])
        twice = jnp.float32(0.0)
        for k in range(listed):
            twice = twice + (near_ref[t, k] == own).astype(jnp.float32)
        selfs = selfs + twice * (mine * mine)
        pull = jnp.where(sub < 4, fold[0] * mine[0:1], fold[1] * mine[4:5])
        pull = pull[0:4] + pull[4:8]
        force_ref[0, :, out_span] = cols[0:3, own_span] * pull[3:4] - pull[0:3]
        return totals, selfs

    def step(m, carry):
        for s in range(UNROLL):
            t = UNROLL * m + s
            before = (s - 1) % UNROLL
            carry = finish(jnp.maximum(t - 1, 0), before, carry)
            geometry(jnp.minimum(t + 1, row_tiles - 1), (s + 1) % UNROLL)
            blocks(t, s)
        return carry

    zero = jnp.zeros((8, TILE), jnp.float32)
    sums[UNROLL - 1][...] = jnp.zeros(sums[UNROLL - 1].shape, jnp.float32)
    geometry(0, 0)
    carry = lax.fori_loop(0, row_tiles // UNROLL, step, (zero, zero))
    twice = jnp.float32(0.0)
    for k in range(listed):
        twice = twice + (near_ref[0, k] == first_tile).astype(jnp.float32)
    first = cols[8:16, pl.ds(pl.multiple_of(first_tile * TILE, TILE), TILE)]
    totals, selfs = finish(row_tiles - 1, UNROLL - 1, carry)
    selfs = selfs - twice * (first * first)
    soft = rounded(lax.rsqrt(jnp.full((8, TILE), DELTA_SOFT, jnp.float32)))
    sub = rows_of(TILE)
    both = totals - jnp.where(sub < 4, selfs * soft, 0.0)
    lane1 = lax.broadcasted_iota(jnp.int32, (1, TILE), 1)
    line = jnp.zeros((1, TILE), jnp.float32)
    for h in range(3):
        value = jnp.sum(both[h : h + 1] + both[4 + h : 5 + h])
        line = jnp.where(lane1 == h, value, line)
    energy_ref[...] = line


def per_device(
    coords, velocities, coupling, charges, types, type_sigma, type_eps, near_tiles, accept
):
    parts, width = lax.axis_size("atom"), coords.shape[2]
    atoms = parts * width
    part = lax.axis_index("atom")
    packed = jnp.concatenate([coords, velocities, coupling], axis=1)
    rows = jnp.concatenate([coords, coupling], axis=1)
    lower, upper = moved(packed, 1, 0), moved(packed, -1, 0)
    halves = [rows] + [moved(rows, 0, step) for step in range(1, parts)]
    for by, block in ((1, lower), (-1, upper)):
        halves.append(block)
        for step in range(1, parts):
            halves.append(moved(coupling, by, step))

    smem = pl.BlockSpec(memory_space=pltpu.SMEM)
    vmem = pl.BlockSpec(memory_space=pltpu.VMEM)
    pairs = width * near_tiles.shape[1] * TILE
    force, line = pl.pallas_call(
        partial(tiles_kernel, parts, near_tiles.shape[1]),
        out_shape=(
            jax.ShapeDtypeStruct(coords.shape, jnp.float32),
            jax.ShapeDtypeStruct((1, TILE), jnp.float32),
        ),
        in_specs=[smem] * 4 + [vmem] * (2 + len(halves)),
        out_specs=(vmem, vmem),
        scratch_shapes=[
            pltpu.VMEM((16, atoms), jnp.float32),
            pltpu.VMEM((atoms, DEPTH), jnp.bfloat16),
            pltpu.VMEM((DEPTH, COLS * width), jnp.bfloat16),
            pltpu.VMEM((16, atoms), jnp.bfloat16),
            pltpu.VMEM((16, atoms), jnp.bfloat16),
        ]
        + [pltpu.VMEM((near_tiles.shape[1], TILE, COLS * TILE), jnp.float32)] * UNROLL
        + [pltpu.VMEM((3, 16, 2 * TILE), jnp.float32)] * UNROLL,
        cost_estimate=pl.CostEstimate(
            flops=50 * pairs, bytes_accessed=4 * 20 * atoms, transcendentals=2 * pairs
        ),
        name="tiles",
    )(
        part.reshape(1).astype(jnp.int32),
        near_tiles,
        type_sigma,
        type_eps,
        charges.reshape(1, atoms),
        types.reshape(1, atoms),
        *halves,
    )
    shares = jnp.stack([line[0, :3]] + [moved(line, 0, step)[0, :3] for step in range(1, parts)])
    total = shares[0]
    for step in range(1, parts):
        total = total + shares[step]
    if parts > 2:
        order = (jnp.arange(parts) - part) % parts
        total = jnp.sum(shares[order], axis=0)
    energies = (total * (0.5 / atoms))[None]

    replica, cycle = lax.axis_index("lam"), lax.axis_size("lam")
    up = accept[replica] == 1
    low = accept[(replica + cycle - 1) % cycle] == 1
    new_coords = jnp.where(up, upper[:, 0:3], jnp.where(low, lower[:, 0:3], coords))
    new_velocities = jnp.where(up, upper[:, 3:6], jnp.where(low, lower[:, 3:6], velocities))
    return (energies, force, new_coords, new_velocities)


def solution(mesh):
    split = P("lam", None, "atom")
    return jax.shard_map(
        per_device,
        mesh=mesh,
        in_specs=(split, split, split, P(), P(), P(), P(), P("atom", None), P()),
        out_specs=(P("lam", None), split, split, split),
        check_vma=False,
    )
```

```python
import math
from functools import partial

import jax
import jax.numpy as jnp
from jax import lax
from jax.experimental import pallas as pl
from jax.experimental.pallas import tpu as pltpu
from jax.sharding import PartitionSpec as P

TILE = 128
DELTA_SOFT = 0.05
SUB = 16
DEPTH = 32
COLS = 2
UNROLL = 8
GROUP = 8
MESH = pl.DeviceIdType.MESH


def halved(x):
    high = x.astype(jnp.bfloat16)
    low = x - high.astype(jnp.float32)
    return jnp.concatenate([high, low.astype(jnp.bfloat16)], axis=1)


def rounded(x):
    return x.astype(jnp.bfloat16).astype(jnp.float32)


def tiles_kernel(
    parts, listed, near_ref, sigma_ref, eps_ref, accept_ref, charges_ref, types_ref, coords_ref, velocities_ref,
    coupling_ref, energy_ref, force_ref, new_coords_ref, new_velocities_ref, cols, near_feat, own_feat, lhs_e, lhs_f,
    far_coords, far_coupling, lam_coupling, lam_coords, lam_velocities, share, far_share,
    send_part, recv_part, send_lam, recv_lam, send_more, recv_more, *rest
):
    unroll = len(rest) // 2
    geos, sums = rest[:unroll], rest[unroll:]
    width = coords_ref.shape[2]
    atoms = cols.shape[1]
    row_tiles = width // TILE
    cycle = lax.axis_size("lam")
    replica, part = lax.axis_index("lam"), lax.axis_index("atom")
    first_tile = part * row_tiles
    upper, lower = lax.rem(replica + 1, cycle), lax.rem(replica + cycle - 1, cycle)

    def place(r, p):
        return {"lam": r, "atom": p}

    def copy(src, dst, send, recv, target):
        return pltpu.make_async_remote_copy(
            src_ref=src, dst_ref=dst, send_sem=send, recv_sem=recv, device_id=target, device_id_type=MESH
        )

    def partner(step):
        return place(replica, lax.rem(part + parts - step, parts))

    sides = (place(upper, part), place(lower, part))
    barrier = pltpu.get_barrier_semaphore()
    greeted = [partner(step) for step in range(1, parts)] + list(sides)
    for target in greeted:
        pl.semaphore_signal(barrier, inc=1, device_id=target, device_id_type=MESH)

    kinds = types_ref[...]
    radius = jnp.zeros(kinds.shape, jnp.float32)
    depth = jnp.zeros(kinds.shape, jnp.float32)
    for level in range(sigma_ref.shape[0]):
        here = kinds == level
        radius = jnp.where(here, sigma_ref[level], radius)
        depth = jnp.where(here, eps_ref[level], depth)
    cols[3:4, :] = 0.5 * radius
    base = 2.0 * jnp.sqrt(depth)
    for row in (11, 15):
        cols[row : row + 1, :] = jnp.zeros((1, atoms), jnp.float32)
    for h in range(3):
        cols[8 + h : 9 + h, :] = charges_ref[...]
        cols[12 + h : 13 + h, :] = base
    spans = []
    for step in range(parts):
        start = pl.multiple_of(lax.rem(part + step, parts) * width, TILE)
        spans.append(pl.ds(start, width))

    pl.semaphore_wait(barrier, len(greeted))
    far_c = [
        copy(coupling_ref, far_coupling.at[step - 1], send_part.at[0, step - 1], recv_part.at[0, step - 1], partner(step))
        for step in range(1, parts)
    ]
    far_x = [
        copy(coords_ref, far_coords.at[step - 1], send_part.at[1, step - 1], recv_part.at[1, step - 1], partner(step))
        for step in range(1, parts)
    ]
    near_c = [
        [
            copy(
                coupling_ref if step == 0 else far_coupling.at[step - 1],
                lam_coupling.at[side, step],
                send_lam.at[side, step],
                recv_lam.at[side, step],
                sides[side],
            )
            for step in range(parts)
        ]
        for side in range(2)
    ]
    swaps = [
        copy(src, dst.at[side], send_more.at[i, side], recv_more.at[i, side], sides[side])
        for side in range(2)
        for i, (src, dst) in enumerate(((coords_ref, lam_coords), (velocities_ref, lam_velocities)))
    ]
    for c in far_c:
        c.start()
    for side in range(2):
        near_c[side][0].start()
    for c in far_x:
        c.start()

    def set_coords(step, ref):
        for c in range(3):
            cols[c : c + 1, spans[step]] = ref[c] - 0.5

    def set_coupling(h, step, ref):
        for c, row in ((0, 8 + h), (1, 12 + h)):
            cols[row : row + 1, spans[step]] = cols[row : row + 1, spans[step]] * ref[c]

    set_coords(0, coords_ref)
    set_coupling(0, 0, coupling_ref)

    def rows_of(n):
        return lax.broadcasted_iota(jnp.int32, (8, n), 0)

    def base_rows(span):
        four = cols[0:4, span]
        return jnp.concatenate([four, four], axis=0)

    def thirds(x):
        high = rounded(x)
        low = x - high
        mid = rounded(low)
        return high, mid, low - mid

    def near_part(c):
        span = pl.ds(pl.multiple_of(c * TILE, TILE), TILE)
        sub = rows_of(TILE)
        quad = sub % 4
        f8 = base_rows(span)
        high, mid, low = thirds(f8)
        sign = jnp.where(quad == 3, 2.0, -2.0).astype(jnp.float32)
        square = f8 * f8
        norm = square[0:1] + square[1:2] + square[2:3]
        mixed = jnp.where(sub < 3, norm, square[3:4])
        nh, nm, nl = thirds(mixed)
        last = jnp.where(quad == 0, nh, jnp.where(quad == 1, nm, nl))
        last = jnp.where(sub == 3, nh, jnp.where(sub == 4, nm, last))
        last = jnp.where(sub >= 5, 1.0, last)
        feats = jnp.concatenate([high * sign, mid * sign, jnp.where(sub < 4, high, low) * sign, last], axis=0)
        near_feat[c] = feats.astype(jnp.bfloat16).T

    def near_half(step):
        offset = lax.rem(part + step, parts) * row_tiles

        def some(c, carry):
            for i in range(GROUP):
                near_part(offset + GROUP * c + i)
            return carry

        lax.fori_loop(0, row_tiles // GROUP, some, 0)

    def lhs_part(c):
        span = pl.ds(pl.multiple_of(c * TILE, TILE), TILE)
        sub = rows_of(TILE)
        quad = sub % 4
        f8 = base_rows(span)
        own8 = cols[8:16, span]
        oh = rounded(own8)
        lhs_e[c] = jnp.concatenate([oh, own8 - oh], axis=0).astype(jnp.bfloat16)
        pos = jnp.where(quad == 3, 1.0, f8)
        scale = jnp.where(sub < 4, own8[0:1], 6.0 * own8[4:5])
        wide = pos * scale
        wh = rounded(wide)
        lhs_f[c] = jnp.concatenate([wh, wide - wh], axis=0).astype(jnp.bfloat16)

    def lhs_parts(c, carry):
        for i in range(GROUP):
            lhs_part(GROUP * c + i)
        return carry

    def own_part(c):
        span = pl.ds(pl.multiple_of((first_tile + c) * TILE, TILE), TILE)
        sub = rows_of(TILE)
        quad = sub % 4
        f8 = base_rows(span)
        high, mid, low = thirds(f8)
        square = f8 * f8
        norm = square[0:1] + square[1:2] + square[2:3]
        first = jnp.where(sub < 4, high, mid)
        third = jnp.where(sub < 4, low, high)
        outs = []
        for which in range(COLS):
            const = (norm + DELTA_SOFT, norm + square[3:4], square[3:4])[which]
            ch, cm, cl = thirds(const)
            ones = sub < (3, 5, 5)[which]
            if which == 2:
                ones = (sub == 3) | (sub == 4)
            last = jnp.where(ones, 1.0, 0.0)
            last = jnp.where(sub == 5, ch, jnp.where(sub == 6, cm, jnp.where(sub == 7, cl, last)))
            keep = (quad != 3, quad <= 3, quad == 3)[which]
            a = jnp.where(keep, first, 0.0)
            outs.append(jnp.concatenate([a, a, jnp.where(keep, third, 0.0), last], axis=0))
        spot = pl.ds(pl.multiple_of(c * (COLS * TILE), TILE), COLS * TILE)
        own_feat[:, spot] = jnp.concatenate(outs, axis=1).astype(jnp.bfloat16)

    def own_parts(c, carry):
        for i in range(GROUP):
            own_part(GROUP * c + i)
        return carry

    lax.fori_loop(0, row_tiles // GROUP, own_parts, 0)
    near_half(0)
    for step in range(1, parts):
        far_c[step - 1].wait_recv()
        for side in range(2):
            near_c[side][step].start()
    for c in swaps:
        c.start()
    for step in range(1, parts):
        set_coupling(0, step, far_coupling.at[step - 1])
        far_x[step - 1].wait_recv()
        set_coords(step, far_coords.at[step - 1])
        near_half(step)
    for side, h in ((0, 1), (1, 2)):
        for step in range(parts):
            near_c[side][step].wait_recv()
            set_coupling(h, step, lam_coupling.at[side, step])
    lax.fori_loop(0, atoms // (GROUP * TILE), lhs_parts, 0)

    def geometry(t, s):
        spot = pl.ds(pl.multiple_of(t * (COLS * TILE), TILE), COLS * TILE)
        rhs = own_feat[:, spot]
        for k in range(listed):
            geos[s][k] = jnp.dot(near_feat[near_ref[k, t]], rhs, preferred_element_type=jnp.float32)

    def blocks(t, s):
        total = None
        for k in range(listed):
            invs, charge, ljs, well = [], [], [], []
            for b in range(TILE // SUB):
                rows = pl.ds(b * SUB, SUB)
                inv = lax.rsqrt(geos[s][k, rows, 0:TILE])
                charge.append(halved(inv * (inv * inv)))
                invs.append(inv.astype(jnp.bfloat16))
            for b in range(TILE // SUB):
                rows = pl.ds(b * SUB, SUB)
                both = geos[s][k, rows, TILE : 2 * TILE]
                root = lax.rsqrt(both)
                p = root * root
                if COLS == 3:
                    x = geos[s][k, rows, 2 * TILE : 3 * TILE] * p
                else:
                    x = ((both - geos[s][k, rows, 0:TILE]) + DELTA_SOFT) * p
                x3 = x * x * x
                low = x3 - 1.0
                ljs.append((x3 * low).astype(jnp.bfloat16))
                well.append(halved((x3 * p) * (x3 + low)))
            le = lhs_e[near_ref[k, t]]
            lf = lhs_f[near_ref[k, t]]
            fc = jnp.dot(lf, jnp.concatenate(charge, axis=0), preferred_element_type=jnp.float32)
            fw = jnp.dot(lf, jnp.concatenate(well, axis=0), preferred_element_type=jnp.float32)
            pairs = jnp.concatenate([jnp.concatenate(invs, axis=0), jnp.concatenate(ljs, axis=0)], axis=1)
            en = jnp.dot(le, pairs, preferred_element_type=jnp.float32)
            new = (fc, fw, en)
            total = new if total is None else tuple(x + y for x, y in zip(total, new))
        for i, x in enumerate(total):
            sums[s][i] = x

    def own_hits(t):
        hits = jnp.int32(0)
        for k in range(listed):
            away = near_ref[k, t] - (first_tile + t)
            hits = hits + 1 - jnp.minimum(away * away, 1)
        return jnp.full((8, TILE), hits, jnp.int32).astype(jnp.float32)

    def finish(t, s, carry):
        totals, selfs = carry
        own = first_tile + t
        own_span = pl.ds(pl.multiple_of(own * TILE, TILE), TILE)
        out_span = pl.ds(pl.multiple_of(t * TILE, TILE), TILE)
        sub = rows_of(TILE)
        quad = sub % 4
        mine = cols[8:16, own_span]
        fold = []
        for i in range(2):
            x = sums[s][i, 0:8] + sums[s][i, 8:16]
            fold.append(x[:, :TILE] + x[:, TILE:])
        en = sums[s][2, 0:8] + sums[s][2, 8:16]
        totals = totals + mine * jnp.where(sub < 4, en[:, :TILE], en[:, TILE:])
        selfs = selfs + own_hits(t) * (mine * mine)
        pull = jnp.where(sub < 4, fold[0] * mine[0:1], fold[1] * mine[4:5])
        pull = pull[0:4] + pull[4:8]
        force = cols[0:3, own_span] * pull[3:4] - pull[0:3]
        for c in range(3):
            force_ref[c, :, out_span] = force[c : c + 1]
        return totals, selfs

    def step(m, carry):
        for s in range(unroll):
            t = unroll * m + s
            before = (s - 1) % unroll
            carry = finish(jnp.maximum(t - 1, 0), before, carry)
            geometry(jnp.minimum(t + 1, row_tiles - 1), (s + 1) % unroll)
            blocks(t, s)
        return carry

    zero = jnp.zeros((8, TILE), jnp.float32)
    sums[unroll - 1][...] = jnp.zeros(sums[unroll - 1].shape, jnp.float32)
    geometry(0, 0)
    carry = lax.fori_loop(0, row_tiles // unroll, step, (zero, zero))
    first = cols[8:16, pl.ds(pl.multiple_of(first_tile * TILE, TILE), TILE)]
    totals, selfs = finish(row_tiles - 1, unroll - 1, carry)
    selfs = selfs - own_hits(0) * (first * first)
    soft = rounded(lax.rsqrt(jnp.full((8, TILE), DELTA_SOFT, jnp.float32)))
    sub = rows_of(TILE)
    share[...] = totals - jnp.where(sub < 4, selfs * soft, 0.0)

    for c in swaps:
        c.wait_recv()
    up = accept_ref[replica]
    low = accept_ref[lower]

    def swapped(out, ref, got):
        for c in range(3):
            up_flag = jnp.full((1, width), up, jnp.int32) == 1
            low_flag = jnp.full((1, width), low, jnp.int32) == 1
            out[c] = jnp.where(up_flag, got[1, c], jnp.where(low_flag, got[0, c], ref[c]))

    swapped(new_coords_ref, coords_ref, lam_coords)
    far_e = [
        copy(share, far_share.at[step - 1], send_part.at[2, step - 1], recv_part.at[2, step - 1], partner(step))
        for step in range(1, parts)
    ]
    for c in far_e:
        c.start()
    swapped(new_velocities_ref, velocities_ref, lam_velocities)
    for c in far_c + far_x + near_c[0] + near_c[1] + swaps:
        c.wait_send()
    for c in far_e:
        c.wait()
    both = share[...]
    if parts == 2:
        both = both + far_share[0]
    elif parts > 2:
        both = jnp.zeros_like(both)
        for p in range(parts):
            for step in range(parts):
                here = jnp.full((8, TILE), lax.rem(part + step, parts), jnp.int32) == p
                both = both + jnp.where(here, share[...] if step == 0 else far_share[step - 1], 0.0)
    lane1 = lax.broadcasted_iota(jnp.int32, (1, TILE), 1)
    line = jnp.zeros((1, TILE), jnp.float32)
    for h in range(3):
        value = jnp.sum(both[h : h + 1] + both[4 + h : 5 + h])
        line = jnp.where(lane1 == h, value * (0.5 / atoms), line)
    energy_ref[...] = line


def per_device(
    coords, velocities, coupling, charges, types, type_sigma, type_eps, near_tiles, accept
):
    parts, width = lax.axis_size("atom"), coords.shape[2]
    atoms = parts * width
    listed = near_tiles.shape[1]
    unroll = math.gcd(width // TILE, UNROLL)
    smem = pl.BlockSpec(memory_space=pltpu.SMEM)
    vmem = pl.BlockSpec(memory_space=pltpu.VMEM)
    f32, bf16, far = jnp.float32, jnp.bfloat16, max(parts - 1, 1)
    dma = pltpu.SemaphoreType.DMA
    rows = jax.ShapeDtypeStruct((3, 1, width), f32)
    line, force, new_coords, new_velocities = pl.pallas_call(
        partial(tiles_kernel, parts, listed),
        out_shape=(jax.ShapeDtypeStruct((1, TILE), f32), rows, rows, rows),
        in_specs=[smem] * 4 + [vmem] * 5,
        out_specs=(vmem,) * 4,
        scratch_shapes=[
            pltpu.VMEM((16, atoms), f32),
            pltpu.VMEM((atoms // TILE, TILE, DEPTH), bf16),
            pltpu.VMEM((DEPTH, COLS * width), bf16),
            pltpu.VMEM((atoms // TILE, 16, TILE), bf16),
            pltpu.VMEM((atoms // TILE, 16, TILE), bf16),
            pltpu.VMEM((far, 3, 1, width), f32),
            pltpu.VMEM((far, 2, 1, width), f32),
            pltpu.VMEM((2, parts, 2, 1, width), f32),
            pltpu.VMEM((2, 3, 1, width), f32),
            pltpu.VMEM((2, 3, 1, width), f32),
            pltpu.VMEM((8, TILE), f32),
            pltpu.VMEM((far, 8, TILE), f32),
            dma((3, far)),
            dma((3, far)),
            dma((2, parts)),
            dma((2, parts)),
            dma((2, 2)),
            dma((2, 2)),
        ]
        + [pltpu.VMEM((listed, TILE, COLS * TILE), f32)] * unroll
        + [pltpu.VMEM((3, 16, 2 * TILE), f32)] * unroll,
        compiler_params=pltpu.CompilerParams(collective_id=0, has_side_effects=True),
        name="tiles",
    )(
        near_tiles.T,
        type_sigma,
        type_eps,
        accept,
        charges.reshape(1, atoms),
        types.reshape(1, atoms),
        *(x.transpose(1, 0, 2) for x in (coords, velocities, coupling)),
    )
    return (line[:, :3], *(x.transpose(1, 0, 2) for x in (force, new_coords, new_velocities)))


def solution(mesh):
    split = P("lam", None, "atom")
    return jax.shard_map(
        per_device,
        mesh=mesh,
        in_specs=(split, split, split, P(), P(), P(), P(), P("atom", None), P()),
        out_specs=(P("lam", None), split, split, split),
        check_vma=False,
    )
```

```python
import math
from functools import partial

import jax
import jax.numpy as jnp
from jax import lax
from jax.experimental import pallas as pl
from jax.experimental.pallas import tpu as pltpu
from jax.sharding import PartitionSpec as P

TILE = 128
DELTA_SOFT = 0.05
SUB = 16
DEPTH = 32
COLS = 2
UNROLL = 8
GROUP = 8
MESH = pl.DeviceIdType.MESH


def halved(x):
    high = x.astype(jnp.bfloat16)
    low = x - high.astype(jnp.float32)
    return jnp.concatenate([high, low.astype(jnp.bfloat16)], axis=1)


def rounded(x):
    return x.astype(jnp.bfloat16).astype(jnp.float32)


def tiles_kernel(
    parts, listed, near_ref, sigma_ref, eps_ref, accept_ref, charges_hbm, types_hbm, coords_hbm,
    velocities_hbm, coupling_hbm, energy_ref, force_out, new_coords_out, new_velocities_out, charges_ref, types_ref,
    coords_ref, velocities_ref, coupling_ref, force_ref, new_coords_ref, new_velocities_ref, own_sem, out_sem, cols, near_feat, own_feat, lhs_e, lhs_f,
    far_coords, far_coupling, lam_coupling, lam_coords, lam_velocities, share, far_share,
    send_part, recv_part, send_lam, recv_lam, send_more, recv_more, *rest
):
    unroll = len(rest) // 2
    geos, sums = rest[:unroll], rest[unroll:]
    width = coords_ref.shape[2]
    atoms = cols.shape[1]
    row_tiles = width // TILE
    cycle = lax.axis_size("lam")
    replica, part = lax.axis_index("lam"), lax.axis_index("atom")
    first_tile = part * row_tiles
    upper, lower = lax.rem(replica + 1, cycle), lax.rem(replica + cycle - 1, cycle)

    def place(r, p):
        return {"lam": r, "atom": p}

    def copy(src, dst, send, recv, target):
        return pltpu.make_async_remote_copy(
            src_ref=src, dst_ref=dst, send_sem=send, recv_sem=recv, device_id=target, device_id_type=MESH
        )

    def partner(step):
        return place(replica, lax.rem(part + parts - step, parts))

    sides = (place(upper, part), place(lower, part))
    barrier = pltpu.get_barrier_semaphore()
    greeted = [partner(step) for step in range(1, parts)] + list(sides)
    for target in greeted:
        pl.semaphore_signal(barrier, inc=1, device_id=target, device_id_type=MESH)

    own_refs = (
        (types_hbm, types_ref),
        (coords_hbm, coords_ref),
        (charges_hbm, charges_ref),
        (coupling_hbm, coupling_ref),
        (velocities_hbm, velocities_ref),
    )
    owned = [pltpu.make_async_copy(src, dst, own_sem.at[i]) for i, (src, dst) in enumerate(own_refs)]
    for c in owned:
        c.start()
    owned[0].wait()
    kinds = types_ref[...]
    radius = jnp.zeros(kinds.shape, jnp.float32)
    depth = jnp.zeros(kinds.shape, jnp.float32)
    for level in range(sigma_ref.shape[0]):
        here = kinds == level
        radius = jnp.where(here, sigma_ref[level], radius)
        depth = jnp.where(here, eps_ref[level], depth)
    cols[3:4, :] = 0.5 * radius
    base = 2.0 * jnp.sqrt(depth)
    for row in (11, 15):
        cols[row : row + 1, :] = jnp.zeros((1, atoms), jnp.float32)
    owned[2].wait()
    for h in range(3):
        cols[8 + h : 9 + h, :] = charges_ref[...]
        cols[12 + h : 13 + h, :] = base
    spans = []
    for step in range(parts):
        start = pl.multiple_of(lax.rem(part + step, parts) * width, TILE)
        spans.append(pl.ds(start, width))

    def set_coords(step, ref):
        for c in range(3):
            cols[c : c + 1, spans[step]] = ref[c] - 0.5

    def set_coupling(h, step, ref):
        for c, row in ((0, 8 + h), (1, 12 + h)):
            cols[row : row + 1, spans[step]] = cols[row : row + 1, spans[step]] * ref[0, c : c + 1]

    owned[1].wait()
    set_coords(0, coords_ref)
    owned[3].wait()
    set_coupling(0, 0, coupling_ref)

    def rows_of(n):
        return lax.broadcasted_iota(jnp.int32, (8, n), 0)

    def base_rows(span):
        four = cols[0:4, span]
        return jnp.concatenate([four, four], axis=0)

    def thirds(x):
        high = rounded(x)
        low = x - high
        mid = rounded(low)
        return high, mid, low - mid

    def near_part(c):
        span = pl.ds(pl.multiple_of(c * TILE, TILE), TILE)
        sub = rows_of(TILE)
        quad = sub % 4
        f8 = base_rows(span)
        high, mid, low = thirds(f8)
        sign = jnp.where(quad == 3, 2.0, -2.0).astype(jnp.float32)
        square = f8 * f8
        norm = square[0:1] + square[1:2] + square[2:3]
        mixed = jnp.where(sub < 3, norm, square[3:4])
        nh, nm, nl = thirds(mixed)
        last = jnp.where(quad == 0, nh, jnp.where(quad == 1, nm, nl))
        last = jnp.where(sub == 3, nh, jnp.where(sub == 4, nm, last))
        last = jnp.where(sub >= 5, 1.0, last)
        feats = jnp.concatenate([high * sign, mid * sign, jnp.where(sub < 4, high, low) * sign, last], axis=0)
        near_feat[c] = feats.astype(jnp.bfloat16).T

    def near_half(step):
        offset = lax.rem(part + step, parts) * row_tiles

        def some(c, carry):
            for i in range(GROUP):
                near_part(offset + GROUP * c + i)
            return carry

        lax.fori_loop(0, row_tiles // GROUP, some, 0)

    def lhs_part(c):
        span = pl.ds(pl.multiple_of(c * TILE, TILE), TILE)
        sub = rows_of(TILE)
        quad = sub % 4
        f8 = base_rows(span)
        own8 = cols[8:16, span]
        oh = rounded(own8)
        lhs_e[c] = jnp.concatenate([oh, own8 - oh], axis=0).astype(jnp.bfloat16)
        pos = jnp.where(quad == 3, 1.0, f8)
        scale = jnp.where(sub < 4, own8[0:1], 6.0 * own8[4:5])
        wide = pos * scale
        wh = rounded(wide)
        lhs_f[c] = jnp.concatenate([wh, wide - wh], axis=0).astype(jnp.bfloat16)

    def lhs_parts(c, carry):
        for i in range(GROUP):
            lhs_part(GROUP * c + i)
        return carry

    def own_part(c):
        span = pl.ds(pl.multiple_of((first_tile + c) * TILE, TILE), TILE)
        sub = rows_of(TILE)
        quad = sub % 4
        f8 = base_rows(span)
        high, mid, low = thirds(f8)
        square = f8 * f8
        norm = square[0:1] + square[1:2] + square[2:3]
        first = jnp.where(sub < 4, high, mid)
        third = jnp.where(sub < 4, low, high)
        outs = []
        for which in range(COLS):
            const = (norm + DELTA_SOFT, norm + square[3:4], square[3:4])[which]
            ch, cm, cl = thirds(const)
            ones = sub < (3, 5, 5)[which]
            if which == 2:
                ones = (sub == 3) | (sub == 4)
            last = jnp.where(ones, 1.0, 0.0)
            last = jnp.where(sub == 5, ch, jnp.where(sub == 6, cm, jnp.where(sub == 7, cl, last)))
            keep = (quad != 3, quad <= 3, quad == 3)[which]
            a = jnp.where(keep, first, 0.0)
            outs.append(jnp.concatenate([a, a, jnp.where(keep, third, 0.0), last], axis=0))
        spot = pl.ds(pl.multiple_of(c * (COLS * TILE), TILE), COLS * TILE)
        own_feat[:, spot] = jnp.concatenate(outs, axis=1).astype(jnp.bfloat16)

    def own_parts(c, carry):
        for i in range(GROUP):
            own_part(GROUP * c + i)
        return carry

    lax.fori_loop(0, row_tiles // GROUP, own_parts, 0)
    pl.semaphore_wait(barrier, len(greeted))
    far_c = [
        copy(coupling_ref, far_coupling.at[step - 1], send_part.at[0, step - 1], recv_part.at[0, step - 1], partner(step))
        for step in range(1, parts)
    ]
    far_x = [
        copy(coords_ref, far_coords.at[step - 1], send_part.at[1, step - 1], recv_part.at[1, step - 1], partner(step))
        for step in range(1, parts)
    ]
    near_c = [
        [
            copy(
                coupling_ref if step == 0 else far_coupling.at[step - 1],
                lam_coupling.at[side, step],
                send_lam.at[side, step],
                recv_lam.at[side, step],
                sides[side],
            )
            for step in range(parts)
        ]
        for side in range(2)
    ]
    swaps = [
        copy(src, dst.at[side], send_more.at[i, side], recv_more.at[i, side], sides[side])
        for side in range(2)
        for i, (src, dst) in enumerate(((coords_ref, lam_coords), (velocities_ref, lam_velocities)))
    ]
    for c in far_c:
        c.start()
    for side in range(2):
        near_c[side][0].start()
    for c in far_x:
        c.start()

    near_half(0)
    for step in range(1, parts):
        far_c[step - 1].wait_recv()
        for side in range(2):
            near_c[side][step].start()
    for step in range(1, parts):
        set_coupling(0, step, far_coupling.at[step - 1])
        far_x[step - 1].wait_recv()
        set_coords(step, far_coords.at[step - 1])
        near_half(step)
    for side, h in ((0, 1), (1, 2)):
        for step in range(parts):
            near_c[side][step].wait_recv()
            set_coupling(h, step, lam_coupling.at[side, step])
    owned[4].wait()
    for c in swaps:
        c.start()
    lax.fori_loop(0, atoms // (GROUP * TILE), lhs_parts, 0)

    def geometry(t, s):
        spot = pl.ds(pl.multiple_of(t * (COLS * TILE), TILE), COLS * TILE)
        rhs = own_feat[:, spot]
        for k in range(listed):
            geos[s][k] = jnp.dot(near_feat[near_ref[k, t]], rhs, preferred_element_type=jnp.float32)

    def blocks(t, s):
        total = None
        for k in range(listed):
            invs, charge, ljs, well = [], [], [], []
            for b in range(TILE // SUB):
                rows = pl.ds(b * SUB, SUB)
                inv = lax.rsqrt(geos[s][k, rows, 0:TILE])
                charge.append(halved(inv * (inv * inv)))
                invs.append(inv.astype(jnp.bfloat16))
            for b in range(TILE // SUB):
                rows = pl.ds(b * SUB, SUB)
                both = geos[s][k, rows, TILE : 2 * TILE]
                root = lax.rsqrt(both)
                p = root * root
                if COLS == 3:
                    x = geos[s][k, rows, 2 * TILE : 3 * TILE] * p
                else:
                    x = ((both - geos[s][k, rows, 0:TILE]) + DELTA_SOFT) * p
                x3 = x * x * x
                low = x3 - 1.0
                ljs.append((x3 * low).astype(jnp.bfloat16))
                well.append(halved((x3 * p) * (x3 + low)))
            le = lhs_e[near_ref[k, t]]
            lf = lhs_f[near_ref[k, t]]
            fc = jnp.dot(lf, jnp.concatenate(charge, axis=0), preferred_element_type=jnp.float32)
            fw = jnp.dot(lf, jnp.concatenate(well, axis=0), preferred_element_type=jnp.float32)
            pairs = jnp.concatenate([jnp.concatenate(invs, axis=0), jnp.concatenate(ljs, axis=0)], axis=1)
            en = jnp.dot(le, pairs, preferred_element_type=jnp.float32)
            new = (fc, fw, en)
            total = new if total is None else tuple(x + y for x, y in zip(total, new))
        for i, x in enumerate(total):
            sums[s][i] = x

    def own_hits(t):
        hits = jnp.int32(0)
        for k in range(listed):
            away = near_ref[k, t] - (first_tile + t)
            hits = hits + 1 - jnp.minimum(away * away, 1)
        return jnp.full((8, TILE), hits, jnp.int32).astype(jnp.float32)

    def finish(t, s, carry):
        totals, selfs = carry
        own = first_tile + t
        own_span = pl.ds(pl.multiple_of(own * TILE, TILE), TILE)
        out_span = pl.ds(pl.multiple_of(t * TILE, TILE), TILE)
        sub = rows_of(TILE)
        quad = sub % 4
        mine = cols[8:16, own_span]
        fold = []
        for i in range(2):
            x = sums[s][i, 0:8] + sums[s][i, 8:16]
            fold.append(x[:, :TILE] + x[:, TILE:])
        en = sums[s][2, 0:8] + sums[s][2, 8:16]
        totals = totals + mine * jnp.where(sub < 4, en[:, :TILE], en[:, TILE:])
        selfs = selfs + own_hits(t) * (mine * mine)
        pull = jnp.where(sub < 4, fold[0] * mine[0:1], fold[1] * mine[4:5])
        pull = pull[0:4] + pull[4:8]
        force = cols[0:3, own_span] * pull[3:4] - pull[0:3]
        for c in range(3):
            force_ref[c, :, out_span] = force[c : c + 1]
        return totals, selfs

    def step(m, carry):
        for s in range(unroll):
            t = unroll * m + s
            before = (s - 1) % unroll
            carry = finish(jnp.maximum(t - 1, 0), before, carry)
            geometry(jnp.minimum(t + 1, row_tiles - 1), (s + 1) % unroll)
            blocks(t, s)
        return carry

    zero = jnp.zeros((8, TILE), jnp.float32)
    sums[unroll - 1][...] = jnp.zeros(sums[unroll - 1].shape, jnp.float32)
    geometry(0, 0)
    carry = lax.fori_loop(0, row_tiles // unroll, step, (zero, zero))
    first = cols[8:16, pl.ds(pl.multiple_of(first_tile * TILE, TILE), TILE)]
    totals, selfs = finish(row_tiles - 1, unroll - 1, carry)
    selfs = selfs - own_hits(0) * (first * first)
    soft = rounded(lax.rsqrt(jnp.full((8, TILE), DELTA_SOFT, jnp.float32)))
    sub = rows_of(TILE)
    share[...] = totals - jnp.where(sub < 4, selfs * soft, 0.0)

    outs = [
        pltpu.make_async_copy(src, dst, out_sem.at[i])
        for i, (src, dst) in enumerate(
            ((force_ref, force_out), (new_coords_ref, new_coords_out), (new_velocities_ref, new_velocities_out))
        )
    ]
    for c in swaps:
        c.wait_recv()
    up = accept_ref[replica]
    low = accept_ref[lower]

    def swapped(out, ref, got):
        for c in range(3):
            up_flag = jnp.full((1, width), up, jnp.int32) == 1
            low_flag = jnp.full((1, width), low, jnp.int32) == 1
            out[c] = jnp.where(up_flag, got[1, c], jnp.where(low_flag, got[0, c], ref[c]))

    swapped(new_coords_ref, coords_ref, lam_coords)
    far_e = [
        copy(share, far_share.at[step - 1], send_part.at[2, step - 1], recv_part.at[2, step - 1], partner(step))
        for step in range(1, parts)
    ]
    for c in far_e:
        c.start()
    outs[0].start()
    swapped(new_velocities_ref, velocities_ref, lam_velocities)
    outs[1].start()
    outs[2].start()
    for c in far_c + far_x + near_c[0] + near_c[1] + swaps:
        c.wait_send()
    for c in far_e:
        c.wait()
    both = share[...]
    if parts == 2:
        both = both + far_share[0]
    elif parts > 2:
        both = jnp.zeros_like(both)
        for p in range(parts):
            for step in range(parts):
                here = jnp.full((8, TILE), lax.rem(part + step, parts), jnp.int32) == p
                both = both + jnp.where(here, share[...] if step == 0 else far_share[step - 1], 0.0)
    lane1 = lax.broadcasted_iota(jnp.int32, (1, TILE), 1)
    line = jnp.zeros((1, TILE), jnp.float32)
    for h in range(3):
        value = jnp.sum(both[h : h + 1] + both[4 + h : 5 + h])
        line = jnp.where(lane1 == h, value * (0.5 / atoms), line)
    energy_ref[...] = line
    for c in outs:
        c.wait()


def handed_on(line_ref, *refs):
    half = (len(refs) - 1) // 2
    refs[half][...] = line_ref[:, 0:3]
    for src, dst in zip(refs[:half], refs[half + 1 :]):
        dst[...] = src[...]


def per_device(
    coords, velocities, coupling, charges, types, type_sigma, type_eps, near_tiles, accept
):
    parts, width = lax.axis_size("atom"), coords.shape[2]
    atoms = parts * width
    listed = near_tiles.shape[1]
    unroll = math.gcd(width // TILE, UNROLL)
    smem = pl.BlockSpec(memory_space=pltpu.SMEM)
    vmem = pl.BlockSpec(memory_space=pltpu.VMEM)
    whole = pl.BlockSpec(memory_space=pl.ANY)
    f32, bf16, far = jnp.float32, jnp.bfloat16, max(parts - 1, 1)
    dma = pltpu.SemaphoreType.DMA
    rows = jax.ShapeDtypeStruct((3, 1, width), f32)
    line, force, new_coords, new_velocities = pl.pallas_call(
        partial(tiles_kernel, parts, listed),
        out_shape=(jax.ShapeDtypeStruct((1, TILE), f32), rows, rows, rows),
        in_specs=[smem] * 4 + [whole] * 5,
        out_specs=(vmem,) + (whole,) * 3,
        scratch_shapes=[
            pltpu.VMEM((1, atoms), f32),
            pltpu.VMEM((1, atoms), jnp.int32),
            pltpu.VMEM((3, 1, width), f32),
            pltpu.VMEM((3, 1, width), f32),
            pltpu.VMEM((1, 2, width), f32),
            pltpu.VMEM((3, 1, width), f32),
            pltpu.VMEM((3, 1, width), f32),
            pltpu.VMEM((3, 1, width), f32),
            dma((5,)),
            dma((3,)),
            pltpu.VMEM((16, atoms), f32),
            pltpu.VMEM((atoms // TILE, TILE, DEPTH), bf16),
            pltpu.VMEM((DEPTH, COLS * width), bf16),
            pltpu.VMEM((atoms // TILE, 16, TILE), bf16),
            pltpu.VMEM((atoms // TILE, 16, TILE), bf16),
            pltpu.VMEM((far, 3, 1, width), f32),
            pltpu.VMEM((far, 1, 2, width), f32),
            pltpu.VMEM((2, parts, 1, 2, width), f32),
            pltpu.VMEM((2, 3, 1, width), f32),
            pltpu.VMEM((2, 3, 1, width), f32),
            pltpu.VMEM((8, TILE), f32),
            pltpu.VMEM((far, 8, TILE), f32),
            dma((3, far)),
            dma((3, far)),
            dma((2, parts)),
            dma((2, parts)),
            dma((2, 2)),
            dma((2, 2)),
        ]
        + [pltpu.VMEM((listed, TILE, COLS * TILE), f32)] * unroll
        + [pltpu.VMEM((3, 16, 2 * TILE), f32)] * unroll,
        compiler_params=pltpu.CompilerParams(collective_id=0, has_side_effects=True),
        name="tiles",
    )(
        near_tiles.T,
        type_sigma,
        type_eps,
        accept,
        charges.reshape(1, atoms),
        types.reshape(1, atoms),
        coords.transpose(1, 0, 2),
        velocities.transpose(1, 0, 2),
        coupling,
    )
    energies, *results = pl.pallas_call(
        handed_on,
        out_shape=(jax.ShapeDtypeStruct((1, 3), f32), rows, rows, rows),
        in_specs=[vmem] * 4,
        out_specs=(vmem,) * 4,
        name="handed_on",
    )(line, force, new_coords, new_velocities)
    return (energies, *(x.transpose(1, 0, 2) for x in results))


def solution(mesh):
    split = P("lam", None, "atom")
    return jax.shard_map(
        per_device,
        mesh=mesh,
        in_specs=(split, split, split, P(), P(), P(), P(), P("atom", None), P()),
        out_specs=(P("lam", None), split, split, split),
        check_vma=False,
    )
```

```python
import math
from functools import partial

import jax
import jax.numpy as jnp
from jax import lax
from jax.experimental import pallas as pl
from jax.experimental.pallas import tpu as pltpu
from jax.sharding import PartitionSpec as P

TILE = 128
DELTA_SOFT = 0.05
SUB = 16
DEPTH = 32
COLS = 2
CHUNK = 5
UNROLL = 8
GROUP = 8
WIDE = 16
MESH = pl.DeviceIdType.MESH


def halved(x):
    high = x.astype(jnp.bfloat16)
    low = x - high.astype(jnp.float32)
    return jnp.concatenate([high, low.astype(jnp.bfloat16)], axis=1)


def rounded(x):
    return x.astype(jnp.bfloat16).astype(jnp.float32)


def tiles_kernel(
    parts, listed, near_hbm, sigma_hbm, eps_hbm, accept_hbm, charges_hbm, types_hbm, coords_hbm,
    velocities_hbm, coupling_hbm, energy_ref, force_out, new_coords_out, new_velocities_out, near_ref, sigma_ref, eps_ref, accept_ref, charges_ref, types_ref,
    coords_ref, velocities_ref, coupling_ref, force_ref, new_coords_ref, new_velocities_ref, own_sem, out_sem, cols, near_feat, own_feat, lhs_e, lhs_f,
    far_coords, far_coupling, lam_coupling, lam_coords, lam_velocities, share, far_share,
    send_part, recv_part, send_lam, recv_lam, send_more, recv_more, *rest
):
    unroll = len(rest) // 2
    geos, sums = rest[:unroll], rest[unroll:]
    width = coords_ref.shape[2]
    atoms = cols.shape[1]
    row_tiles = width // TILE
    cycle = lax.axis_size("lam")
    replica, part = lax.axis_index("lam"), lax.axis_index("atom")
    first_tile = part * row_tiles
    upper, lower = lax.rem(replica + 1, cycle), lax.rem(replica + cycle - 1, cycle)

    def place(r, p):
        return {"lam": r, "atom": p}

    def copy(src, dst, send, recv, target):
        return pltpu.make_async_remote_copy(
            src_ref=src, dst_ref=dst, send_sem=send, recv_sem=recv, device_id=target, device_id_type=MESH
        )

    def partner(step):
        return place(replica, lax.rem(part + parts - step, parts))

    sides = (place(upper, part), place(lower, part))
    barrier = pltpu.get_barrier_semaphore()
    greeted = [partner(step) for step in range(1, parts)] + list(sides)
    for target in greeted:
        pl.semaphore_signal(barrier, inc=1, device_id=target, device_id_type=MESH)

    own_refs = (
        (types_hbm, types_ref),
        (coords_hbm, coords_ref),
        (charges_hbm, charges_ref),
        (coupling_hbm, coupling_ref),
        (velocities_hbm, velocities_ref),
        (sigma_hbm, sigma_ref),
        (eps_hbm, eps_ref),
        (near_hbm, near_ref),
        (accept_hbm, accept_ref),
    )
    owned = [pltpu.make_async_copy(src, dst, own_sem.at[i]) for i, (src, dst) in enumerate(own_refs)]
    for c in owned:
        c.start()
    owned[0].wait()
    owned[5].wait()
    owned[6].wait()
    kinds = types_ref[...]
    radius = jnp.zeros(kinds.shape, jnp.float32)
    depth = jnp.zeros(kinds.shape, jnp.float32)
    for level in range(sigma_ref.shape[0]):
        here = kinds == level
        radius = jnp.where(here, sigma_ref[level], radius)
        depth = jnp.where(here, eps_ref[level], depth)
    cols[3:4, :] = 0.5 * radius
    base = 2.0 * jnp.sqrt(depth)
    for row in (11, 15):
        cols[row : row + 1, :] = jnp.zeros((1, atoms), jnp.float32)
    owned[2].wait()
    for h in range(3):
        cols[8 + h : 9 + h, :] = charges_ref[...]
        cols[12 + h : 13 + h, :] = base
    spans = []
    for step in range(parts):
        start = pl.multiple_of(lax.rem(part + step, parts) * width, TILE)
        spans.append(pl.ds(start, width))

    def set_coords(step, ref):
        for c in range(3):
            cols[c : c + 1, spans[step]] = ref[c] - 0.5

    def set_coupling(h, step, ref):
        for c, row in ((0, 8 + h), (1, 12 + h)):
            cols[row : row + 1, spans[step]] = cols[row : row + 1, spans[step]] * ref[0, c : c + 1]

    owned[1].wait()
    set_coords(0, coords_ref)
    owned[3].wait()
    set_coupling(0, 0, coupling_ref)

    def rows_of(n):
        return lax.broadcasted_iota(jnp.int32, (8, n), 0)

    def base_rows(span):
        four = cols[0:4, span]
        return jnp.concatenate([four, four], axis=0)

    def thirds(x):
        high = rounded(x)
        low = x - high
        mid = rounded(low)
        return high, mid, low - mid

    def near_part(c):
        span = pl.ds(pl.multiple_of(c * TILE, TILE), TILE)
        sub = rows_of(TILE)
        quad = sub % 4
        f8 = base_rows(span)
        high, mid, low = thirds(f8)
        sign = jnp.where(quad == 3, 2.0, -2.0).astype(jnp.float32)
        square = f8 * f8
        norm = square[0:1] + square[1:2] + square[2:3]
        mixed = jnp.where(sub < 3, norm, square[3:4])
        nh, nm, nl = thirds(mixed)
        last = jnp.where(quad == 0, nh, jnp.where(quad == 1, nm, nl))
        last = jnp.where(sub == 3, nh, jnp.where(sub == 4, nm, last))
        last = jnp.where(sub >= 5, 1.0, last)
        feats = jnp.concatenate([high * sign, mid * sign, jnp.where(sub < 4, high, low) * sign, last], axis=0)
        near_feat[c] = feats.astype(jnp.bfloat16).T

    wide = math.gcd(row_tiles, WIDE)

    def near_half(step):
        offset = lax.rem(part + step, parts) * row_tiles

        def some(c, carry):
            for i in range(wide):
                near_part(offset + wide * c + i)
            return carry

        lax.fori_loop(0, row_tiles // wide, some, 0)

    def lhs_part(c):
        span = pl.ds(pl.multiple_of(c * TILE, TILE), TILE)
        sub = rows_of(TILE)
        quad = sub % 4
        f8 = base_rows(span)
        own8 = cols[8:16, span]
        oh = rounded(own8)
        lhs_e[c] = jnp.concatenate([oh, own8 - oh], axis=0).astype(jnp.bfloat16)
        pos = jnp.where(quad == 3, 1.0, f8)
        scale = jnp.where(sub < 4, own8[0:1], 6.0 * own8[4:5])
        wide = pos * scale
        wh = rounded(wide)
        lhs_f[c] = jnp.concatenate([wh, wide - wh], axis=0).astype(jnp.bfloat16)

    def lhs_parts(c, carry):
        for i in range(GROUP):
            lhs_part(GROUP * c + i)
        return carry

    def own_part(c):
        span = pl.ds(pl.multiple_of((first_tile + c) * TILE, TILE), TILE)
        sub = rows_of(TILE)
        quad = sub % 4
        f8 = base_rows(span)
        high, mid, low = thirds(f8)
        square = f8 * f8
        norm = square[0:1] + square[1:2] + square[2:3]
        first = jnp.where(sub < 4, high, mid)
        third = jnp.where(sub < 4, low, high)
        outs = []
        for which in range(COLS):
            const = (norm + DELTA_SOFT, norm + square[3:4], square[3:4])[which]
            ch, cm, cl = thirds(const)
            ones = sub < (3, 5, 5)[which]
            if which == 2:
                ones = (sub == 3) | (sub == 4)
            last = jnp.where(ones, 1.0, 0.0)
            last = jnp.where(sub == 5, ch, jnp.where(sub == 6, cm, jnp.where(sub == 7, cl, last)))
            keep = (quad != 3, quad <= 3, quad == 3)[which]
            a = jnp.where(keep, first, 0.0)
            outs.append(jnp.concatenate([a, a, jnp.where(keep, third, 0.0), last], axis=0))
        spot = pl.ds(pl.multiple_of(c * (COLS * TILE), TILE), COLS * TILE)
        own_feat[:, spot] = jnp.concatenate(outs, axis=1).astype(jnp.bfloat16)

    def own_parts(c, carry):
        for i in range(GROUP):
            own_part(GROUP * c + i)
        return carry

    lax.fori_loop(0, row_tiles // GROUP, own_parts, 0)
    pl.semaphore_wait(barrier, len(greeted))
    far_c = [
        copy(coupling_ref, far_coupling.at[step - 1], send_part.at[0, step - 1], recv_part.at[0, step - 1], partner(step))
        for step in range(1, parts)
    ]
    far_x = [
        copy(coords_ref, far_coords.at[step - 1], send_part.at[1, step - 1], recv_part.at[1, step - 1], partner(step))
        for step in range(1, parts)
    ]
    near_c = [
        [
            copy(
                coupling_ref if step == 0 else far_coupling.at[step - 1],
                lam_coupling.at[side, step],
                send_lam.at[side, step],
                recv_lam.at[side, step],
                sides[side],
            )
            for step in range(parts)
        ]
        for side in range(2)
    ]
    swaps = [
        copy(src, dst.at[side], send_more.at[i, side], recv_more.at[i, side], sides[side])
        for side in range(2)
        for i, (src, dst) in enumerate(((coords_ref, lam_coords), (velocities_ref, lam_velocities)))
    ]
    for c in far_c:
        c.start()
    for side in range(2):
        near_c[side][0].start()
    for c in far_x:
        c.start()

    near_half(0)
    for step in range(1, parts):
        far_c[step - 1].wait_recv()
        for side in range(2):
            near_c[side][step].start()
    for step in range(1, parts):
        set_coupling(0, step, far_coupling.at[step - 1])
        far_x[step - 1].wait_recv()
        set_coords(step, far_coords.at[step - 1])
        near_half(step)
    for side, h in ((0, 1), (1, 2)):
        for step in range(parts):
            near_c[side][step].wait_recv()
            set_coupling(h, step, lam_coupling.at[side, step])
    owned[4].wait()
    owned[7].wait()
    owned[8].wait()
    for c in swaps:
        c.start()
    lax.fori_loop(0, atoms // (GROUP * TILE), lhs_parts, 0)

    def geometry(t, s):
        spot = pl.ds(pl.multiple_of(t * (COLS * TILE), TILE), COLS * TILE)
        rhs = own_feat[:, spot]
        for k in range(listed):
            geos[s][k] = jnp.dot(near_feat[near_ref[k, t]], rhs, preferred_element_type=jnp.float32)

    def blocks(t, s):
        total = [None] * 3

        def add(i, x):
            total[i] = x if total[i] is None else total[i] + x

        def dot(x, y):
            return jnp.dot(x, y, preferred_element_type=jnp.float32)

        for first in range(0, listed, CHUNK):
            ks = range(first, min(first + CHUNK, listed))
            invs, ljs = [], []
            lf = [lhs_f[near_ref[k, t]] for k in ks]
            le = [lhs_e[near_ref[k, t]] for k in ks]
            charge, well = [], []
            for k in ks:
                for b in range(TILE // SUB):
                    rows = pl.ds(b * SUB, SUB)
                    inv = lax.rsqrt(geos[s][k, rows, 0:TILE])
                    charge.append(halved(inv * (inv * inv)))
                    invs.append(inv.astype(jnp.bfloat16))
            for k in ks:
                for b in range(TILE // SUB):
                    rows = pl.ds(b * SUB, SUB)
                    both = geos[s][k, rows, TILE : 2 * TILE]
                    root = lax.rsqrt(both)
                    p = root * root
                    x = ((both - geos[s][k, rows, 0:TILE]) + DELTA_SOFT) * p
                    x3 = x * x * x
                    low = x3 - 1.0
                    ljs.append((x3 * low).astype(jnp.bfloat16))
                    well.append(halved((x3 * p) * (x3 + low)))
            lfs = jnp.concatenate(lf, axis=1)
            add(0, dot(lfs, jnp.concatenate(charge, axis=0)))
            add(1, dot(lfs, jnp.concatenate(well, axis=0)))
            pairs = jnp.concatenate([jnp.concatenate(invs, axis=0), jnp.concatenate(ljs, axis=0)], axis=1)
            add(2, dot(jnp.concatenate(le, axis=1), pairs))
        for i, x in enumerate(total):
            sums[s][i] = x

    def own_hits(t):
        hits = jnp.int32(0)
        for k in range(listed):
            away = near_ref[k, t] - (first_tile + t)
            hits = hits + 1 - jnp.minimum(away * away, 1)
        return jnp.full((8, TILE), hits, jnp.int32).astype(jnp.float32)

    def finish(t, s, carry):
        totals, selfs = carry
        own = first_tile + t
        own_span = pl.ds(pl.multiple_of(own * TILE, TILE), TILE)
        out_span = pl.ds(pl.multiple_of(t * TILE, TILE), TILE)
        sub = rows_of(TILE)
        quad = sub % 4
        mine = cols[8:16, own_span]
        fold = []
        for i in range(2):
            x = sums[s][i, 0:8] + sums[s][i, 8:16]
            fold.append(x[:, :TILE] + x[:, TILE:])
        en = sums[s][2, 0:8] + sums[s][2, 8:16]
        totals = totals + mine * jnp.where(sub < 4, en[:, :TILE], en[:, TILE:])
        selfs = selfs + own_hits(t) * (mine * mine)
        pull = jnp.where(sub < 4, fold[0] * mine[0:1], fold[1] * mine[4:5])
        pull = pull[0:4] + pull[4:8]
        force = cols[0:3, own_span] * pull[3:4] - pull[0:3]
        for c in range(3):
            force_ref[c, :, out_span] = force[c : c + 1]
        return totals, selfs

    def step(m, carry):
        for s in range(unroll):
            t = unroll * m + s
            before = (s - 1) % unroll
            carry = finish(jnp.maximum(t - 1, 0), before, carry)
            geometry(jnp.minimum(t + 1, row_tiles - 1), (s + 1) % unroll)
            blocks(t, s)
        return carry

    zero = jnp.zeros((8, TILE), jnp.float32)
    sums[unroll - 1][...] = jnp.zeros(sums[unroll - 1].shape, jnp.float32)
    geometry(0, 0)
    carry = lax.fori_loop(0, row_tiles // unroll, step, (zero, zero))
    first = cols[8:16, pl.ds(pl.multiple_of(first_tile * TILE, TILE), TILE)]
    totals, selfs = finish(row_tiles - 1, unroll - 1, carry)
    selfs = selfs - own_hits(0) * (first * first)
    soft = rounded(lax.rsqrt(jnp.full((8, TILE), DELTA_SOFT, jnp.float32)))
    sub = rows_of(TILE)
    share[...] = totals - jnp.where(sub < 4, selfs * soft, 0.0)

    outs = [
        pltpu.make_async_copy(src, dst, out_sem.at[i])
        for i, (src, dst) in enumerate(
            ((force_ref, force_out), (new_coords_ref, new_coords_out), (new_velocities_ref, new_velocities_out))
        )
    ]
    for c in swaps:
        c.wait_recv()
    up = accept_ref[replica]
    low = accept_ref[lower]

    def swapped(out, ref, got):
        for c in range(3):
            up_flag = jnp.full((1, width), up, jnp.int32) == 1
            low_flag = jnp.full((1, width), low, jnp.int32) == 1
            out[c] = jnp.where(up_flag, got[1, c], jnp.where(low_flag, got[0, c], ref[c]))

    swapped(new_coords_ref, coords_ref, lam_coords)
    far_e = [
        copy(share, far_share.at[step - 1], send_part.at[2, step - 1], recv_part.at[2, step - 1], partner(step))
        for step in range(1, parts)
    ]
    for c in far_e:
        c.start()
    outs[0].start()
    swapped(new_velocities_ref, velocities_ref, lam_velocities)
    outs[1].start()
    outs[2].start()
    for c in far_c + far_x + near_c[0] + near_c[1] + swaps:
        c.wait_send()
    for c in far_e:
        c.wait()
    both = share[...]
    if parts == 2:
        both = both + far_share[0]
    elif parts > 2:
        both = jnp.zeros_like(both)
        for p in range(parts):
            for step in range(parts):
                here = jnp.full((8, TILE), lax.rem(part + step, parts), jnp.int32) == p
                both = both + jnp.where(here, share[...] if step == 0 else far_share[step - 1], 0.0)
    lane1 = lax.broadcasted_iota(jnp.int32, (1, TILE), 1)
    line = jnp.zeros((1, TILE), jnp.float32)
    for h in range(3):
        value = jnp.sum(both[h : h + 1] + both[4 + h : 5 + h])
        line = jnp.where(lane1 == h, value * (0.5 / atoms), line)
    energy_ref[...] = line
    for c in outs:
        c.wait()


def handed_on(line_ref, *refs):
    half = (len(refs) - 1) // 2
    refs[half][...] = line_ref[:, 0:3]
    for src, dst in zip(refs[:half], refs[half + 1 :]):
        dst[...] = src[...]


def per_device(
    coords, velocities, coupling, charges, types, type_sigma, type_eps, near_tiles, accept
):
    parts, width = lax.axis_size("atom"), coords.shape[2]
    atoms = parts * width
    listed = near_tiles.shape[1]
    unroll = math.gcd(width // TILE, UNROLL)
    vmem = pl.BlockSpec(memory_space=pltpu.VMEM)
    whole = pl.BlockSpec(memory_space=pl.ANY)
    f32, bf16, far = jnp.float32, jnp.bfloat16, max(parts - 1, 1)
    dma = pltpu.SemaphoreType.DMA
    rows = jax.ShapeDtypeStruct((3, 1, width), f32)
    line, force, new_coords, new_velocities = pl.pallas_call(
        partial(tiles_kernel, parts, listed),
        out_shape=(jax.ShapeDtypeStruct((1, TILE), f32), rows, rows, rows),
        in_specs=[whole] * 9,
        out_specs=(vmem,) + (whole,) * 3,
        scratch_shapes=[
            pltpu.SMEM((listed, width // TILE), jnp.int32),
            pltpu.SMEM(type_sigma.shape, f32),
            pltpu.SMEM(type_eps.shape, f32),
            pltpu.SMEM(accept.shape, jnp.int32),
            pltpu.VMEM((1, atoms), f32),
            pltpu.VMEM((1, atoms), jnp.int32),
            pltpu.VMEM((3, 1, width), f32),
            pltpu.VMEM((3, 1, width), f32),
            pltpu.VMEM((1, 2, width), f32),
            pltpu.VMEM((3, 1, width), f32),
            pltpu.VMEM((3, 1, width), f32),
            pltpu.VMEM((3, 1, width), f32),
            dma((9,)),
            dma((3,)),
            pltpu.VMEM((16, atoms), f32),
            pltpu.VMEM((atoms // TILE, TILE, DEPTH), bf16),
            pltpu.VMEM((DEPTH, COLS * width), bf16),
            pltpu.VMEM((atoms // TILE, 16, TILE), bf16),
            pltpu.VMEM((atoms // TILE, 16, TILE), bf16),
            pltpu.VMEM((far, 3, 1, width), f32),
            pltpu.VMEM((far, 1, 2, width), f32),
            pltpu.VMEM((2, parts, 1, 2, width), f32),
            pltpu.VMEM((2, 3, 1, width), f32),
            pltpu.VMEM((2, 3, 1, width), f32),
            pltpu.VMEM((8, TILE), f32),
            pltpu.VMEM((far, 8, TILE), f32),
            dma((3, far)),
            dma((3, far)),
            dma((2, parts)),
            dma((2, parts)),
            dma((2, 2)),
            dma((2, 2)),
        ]
        + [pltpu.VMEM((listed, TILE, COLS * TILE), f32)] * unroll
        + [pltpu.VMEM((3, 16, 2 * TILE), f32)] * unroll,
        compiler_params=pltpu.CompilerParams(collective_id=0, has_side_effects=True),
        name="tiles",
    )(
        near_tiles.T,
        type_sigma,
        type_eps,
        accept,
        charges.reshape(1, atoms),
        types.reshape(1, atoms),
        coords.transpose(1, 0, 2),
        velocities.transpose(1, 0, 2),
        coupling,
    )
    energies, *results = pl.pallas_call(
        handed_on,
        out_shape=(jax.ShapeDtypeStruct((1, 3), f32), rows, rows, rows),
        in_specs=[vmem] * 4,
        out_specs=(vmem,) * 4,
        name="handed_on",
    )(line, force, new_coords, new_velocities)
    return (energies, *(x.transpose(1, 0, 2) for x in results))


def solution(mesh):
    split = P("lam", None, "atom")
    return jax.shard_map(
        per_device,
        mesh=mesh,
        in_specs=(split, split, split, P(), P(), P(), P(), P("atom", None), P()),
        out_specs=(P("lam", None), split, split, split),
        check_vma=False,
    )
```

```python
import math
from functools import partial

import jax
import jax.numpy as jnp
from jax import lax
from jax.experimental import pallas as pl
from jax.experimental.pallas import tpu as pltpu
from jax.sharding import PartitionSpec as P

TILE = 128
DELTA_SOFT = 0.05
SUB = 16
DEPTH = 32
COLS = 2
CHUNK = 5
UNROLL = 16
PIECES = 1
GROUP = 8
WIDE = 16
MESH = pl.DeviceIdType.MESH


def halved(x):
    high = x.astype(jnp.bfloat16)
    low = x - high.astype(jnp.float32)
    return jnp.concatenate([high, low.astype(jnp.bfloat16)], axis=1)


def rounded(x):
    return x.astype(jnp.bfloat16).astype(jnp.float32)


def tiles_kernel(
    parts, listed, near_hbm, sigma_hbm, eps_hbm, accept_hbm, charges_hbm, types_hbm, coords_hbm,
    velocities_hbm, coupling_hbm, energy_ref, force_out, new_coords_out, new_velocities_out, near_ref, sigma_ref, eps_ref, accept_ref, charges_ref, types_ref,
    coords_ref, velocities_ref, coupling_ref, force_ref, new_coords_ref, new_velocities_ref, own_sem, out_sem, cols, near_feat, own_feat, lhs_e, lhs_f,
    far_coords, far_coupling, lam_coupling, lam_coords, lam_velocities, share, far_share,
    send_part, recv_part, send_x, recv_x, send_lam, recv_lam, send_more, recv_more, *rest
):
    unroll = len(rest) // 2
    geos, sums = rest[:unroll], rest[unroll:]
    width = coords_ref.shape[2]
    atoms = cols.shape[1]
    row_tiles = width // TILE
    cycle = lax.axis_size("lam")
    replica, part = lax.axis_index("lam"), lax.axis_index("atom")
    first_tile = part * row_tiles
    upper, lower = lax.rem(replica + 1, cycle), lax.rem(replica + cycle - 1, cycle)

    def place(r, p):
        return {"lam": r, "atom": p}

    def copy(src, dst, send, recv, target):
        return pltpu.make_async_remote_copy(
            src_ref=src, dst_ref=dst, send_sem=send, recv_sem=recv, device_id=target, device_id_type=MESH
        )

    def partner(step):
        return place(replica, lax.rem(part + parts - step, parts))

    sides = (place(upper, part), place(lower, part))
    barrier = pltpu.get_barrier_semaphore()
    greeted = [partner(step) for step in range(1, parts)] + list(sides)
    for target in greeted:
        pl.semaphore_signal(barrier, inc=1, device_id=target, device_id_type=MESH)

    own_refs = (
        (types_hbm, types_ref),
        (coords_hbm, coords_ref),
        (charges_hbm, charges_ref),
        (coupling_hbm, coupling_ref),
        (velocities_hbm, velocities_ref),
        (sigma_hbm, sigma_ref),
        (eps_hbm, eps_ref),
        (near_hbm, near_ref),
        (accept_hbm, accept_ref),
    )
    owned = [pltpu.make_async_copy(src, dst, own_sem.at[i]) for i, (src, dst) in enumerate(own_refs)]
    for i in (3, 1, 0, 2, 5, 6, 4, 7, 8):
        owned[i].start()
    owned[3].wait()
    owned[1].wait()
    pl.semaphore_wait(barrier, len(greeted))
    far_c = [
        copy(coupling_ref, far_coupling.at[step - 1], send_part.at[0, step - 1], recv_part.at[0, step - 1], partner(step))
        for step in range(1, parts)
    ]
    bit = width // PIECES
    far_x = [
        copy(
            coords_ref.at[:, :, pl.ds(p * bit, bit)],
            far_coords.at[step - 1, :, :, pl.ds(p * bit, bit)],
            send_x.at[p, step - 1],
            recv_x.at[p, step - 1],
            partner(step),
        )
        for step in range(1, parts)
        for p in range(PIECES)
    ]
    near_c = [
        [
            copy(
                coupling_ref if step == 0 else far_coupling.at[step - 1],
                lam_coupling.at[side, step],
                send_lam.at[side, step],
                recv_lam.at[side, step],
                sides[side],
            )
            for step in range(parts)
        ]
        for side in range(2)
    ]
    swaps = [
        copy(src, dst.at[side], send_more.at[i, side], recv_more.at[i, side], sides[side])
        for side in range(2)
        for i, (src, dst) in enumerate(((coords_ref, lam_coords), (velocities_ref, lam_velocities)))
    ]
    for c in far_c:
        c.start()
    for side in range(2):
        near_c[side][0].start()
    for c in far_x:
        c.start()

    owned[0].wait()
    owned[5].wait()
    owned[6].wait()
    kinds = types_ref[...]
    radius = jnp.zeros(kinds.shape, jnp.float32)
    depth = jnp.zeros(kinds.shape, jnp.float32)
    for level in range(sigma_ref.shape[0]):
        here = kinds == level
        radius = jnp.where(here, sigma_ref[level], radius)
        depth = jnp.where(here, eps_ref[level], depth)
    cols[3:4, :] = 0.5 * radius
    base = 2.0 * jnp.sqrt(depth)
    for row in (11, 15):
        cols[row : row + 1, :] = jnp.zeros((1, atoms), jnp.float32)
    owned[2].wait()
    for h in range(3):
        cols[8 + h : 9 + h, :] = charges_ref[...]
        cols[12 + h : 13 + h, :] = base
    spans = []
    for step in range(parts):
        start = pl.multiple_of(lax.rem(part + step, parts) * width, TILE)
        spans.append(pl.ds(start, width))

    def set_coords(step, ref):
        for c in range(3):
            cols[c : c + 1, spans[step]] = ref[c] - 0.5

    def set_coupling(h, step, ref):
        for c, row in ((0, 8 + h), (1, 12 + h)):
            cols[row : row + 1, spans[step]] = cols[row : row + 1, spans[step]] * ref[0, c : c + 1]

    set_coords(0, coords_ref)
    set_coupling(0, 0, coupling_ref)

    def rows_of(n):
        return lax.broadcasted_iota(jnp.int32, (8, n), 0)

    def base_rows(span):
        four = cols[0:4, span]
        return jnp.concatenate([four, four], axis=0)

    def thirds(x):
        high = rounded(x)
        low = x - high
        mid = rounded(low)
        return high, mid, low - mid

    def near_part(c):
        span = pl.ds(pl.multiple_of(c * TILE, TILE), TILE)
        sub = rows_of(TILE)
        quad = sub % 4
        f8 = base_rows(span)
        high, mid, low = thirds(f8)
        sign = jnp.where(quad == 3, 2.0, -2.0).astype(jnp.float32)
        square = f8 * f8
        norm = square[0:1] + square[1:2] + square[2:3]
        mixed = jnp.where(sub < 3, norm, square[3:4])
        nh, nm, nl = thirds(mixed)
        last = jnp.where(quad == 0, nh, jnp.where(quad == 1, nm, nl))
        last = jnp.where(sub == 3, nh, jnp.where(sub == 4, nm, last))
        last = jnp.where(sub >= 5, 1.0, last)
        feats = jnp.concatenate([high * sign, mid * sign, jnp.where(sub < 4, high, low) * sign, last], axis=0)
        near_feat[c] = feats.astype(jnp.bfloat16).T

    wide = math.gcd(row_tiles // PIECES, WIDE)

    def near_half(step, piece=0, pieces=1):
        count = row_tiles // pieces
        offset = lax.rem(part + step, parts) * row_tiles + piece * count

        def some(c, carry):
            for i in range(wide):
                near_part(offset + wide * c + i)
            return carry

        lax.fori_loop(0, count // wide, some, 0)

    def lhs_part(c):
        span = pl.ds(pl.multiple_of(c * TILE, TILE), TILE)
        sub = rows_of(TILE)
        quad = sub % 4
        f8 = base_rows(span)
        own8 = cols[8:16, span]
        oh = rounded(own8)
        lhs_e[c] = jnp.concatenate([oh, own8 - oh], axis=0).astype(jnp.bfloat16)
        pos = jnp.where(quad == 3, 1.0, f8)
        scale = jnp.where(sub < 4, own8[0:1], 6.0 * own8[4:5])
        wide = pos * scale
        wh = rounded(wide)
        lhs_f[c] = jnp.concatenate([wh, wide - wh], axis=0).astype(jnp.bfloat16)

    def lhs_parts(c, carry):
        for i in range(GROUP):
            lhs_part(GROUP * c + i)
        return carry

    def own_part(c):
        span = pl.ds(pl.multiple_of((first_tile + c) * TILE, TILE), TILE)
        sub = rows_of(TILE)
        quad = sub % 4
        f8 = base_rows(span)
        high, mid, low = thirds(f8)
        square = f8 * f8
        norm = square[0:1] + square[1:2] + square[2:3]
        first = jnp.where(sub < 4, high, mid)
        third = jnp.where(sub < 4, low, high)
        outs = []
        for which in range(COLS):
            const = (norm + DELTA_SOFT, norm + square[3:4], square[3:4])[which]
            ch, cm, cl = thirds(const)
            ones = sub < (3, 5, 5)[which]
            if which == 2:
                ones = (sub == 3) | (sub == 4)
            last = jnp.where(ones, 1.0, 0.0)
            last = jnp.where(sub == 5, ch, jnp.where(sub == 6, cm, jnp.where(sub == 7, cl, last)))
            keep = (quad != 3, quad <= 3, quad == 3)[which]
            a = jnp.where(keep, first, 0.0)
            outs.append(jnp.concatenate([a, a, jnp.where(keep, third, 0.0), last], axis=0))
        spot = pl.ds(pl.multiple_of(c * (COLS * TILE), TILE), COLS * TILE)
        own_feat[:, spot] = jnp.concatenate(outs, axis=1).astype(jnp.bfloat16)

    def own_parts(c, carry):
        for i in range(GROUP):
            own_part(GROUP * c + i)
        return carry

    lax.fori_loop(0, row_tiles // GROUP, own_parts, 0)
    near_half(0)
    for step in range(1, parts):
        far_c[step - 1].wait_recv()
        for side in range(2):
            near_c[side][step].start()
    for step in range(1, parts):
        set_coupling(0, step, far_coupling.at[step - 1])
        for p in range(PIECES):
            far_x[(step - 1) * PIECES + p].wait_recv()
            start = pl.multiple_of(lax.rem(part + step, parts) * width + p * bit, TILE)
            for c in range(3):
                cols[c : c + 1, pl.ds(start, bit)] = far_coords[step - 1, c, :, pl.ds(p * bit, bit)] - 0.5
            near_half(step, p, PIECES)
    for side, h in ((0, 1), (1, 2)):
        for step in range(parts):
            near_c[side][step].wait_recv()
            set_coupling(h, step, lam_coupling.at[side, step])
    owned[4].wait()
    owned[7].wait()
    owned[8].wait()
    for c in swaps:
        c.start()
    lax.fori_loop(0, atoms // (GROUP * TILE), lhs_parts, 0)

    def geometry(t, s):
        spot = pl.ds(pl.multiple_of(t * (COLS * TILE), TILE), COLS * TILE)
        rhs = own_feat[:, spot]
        for k in range(listed):
            geos[s][k] = jnp.dot(near_feat[near_ref[k, t]], rhs, preferred_element_type=jnp.float32)

    def blocks(t, s):
        total = [None] * 3

        def add(i, x):
            total[i] = x if total[i] is None else total[i] + x

        def dot(x, y):
            return jnp.dot(x, y, preferred_element_type=jnp.float32)

        for first in range(0, listed, CHUNK):
            ks = range(first, min(first + CHUNK, listed))
            invs, ljs = [], []
            lf = [lhs_f[near_ref[k, t]] for k in ks]
            le = [lhs_e[near_ref[k, t]] for k in ks]
            charge, well = [], []
            for k in ks:
                for b in range(TILE // SUB):
                    rows = pl.ds(b * SUB, SUB)
                    inv = lax.rsqrt(geos[s][k, rows, 0:TILE])
                    charge.append(halved(inv * (inv * inv)))
                    invs.append(inv.astype(jnp.bfloat16))
            for k in ks:
                for b in range(TILE // SUB):
                    rows = pl.ds(b * SUB, SUB)
                    both = geos[s][k, rows, TILE : 2 * TILE]
                    root = lax.rsqrt(both)
                    p = root * root
                    x = ((both - geos[s][k, rows, 0:TILE]) + DELTA_SOFT) * p
                    x3 = x * x * x
                    low = x3 - 1.0
                    ljs.append((x3 * low).astype(jnp.bfloat16))
                    well.append(halved((x3 * p) * (x3 + low)))
            lfs = jnp.concatenate(lf, axis=1)
            add(0, dot(lfs, jnp.concatenate(charge, axis=0)))
            add(1, dot(lfs, jnp.concatenate(well, axis=0)))
            pairs = jnp.concatenate([jnp.concatenate(invs, axis=0), jnp.concatenate(ljs, axis=0)], axis=1)
            add(2, dot(jnp.concatenate(le, axis=1), pairs))
        for i, x in enumerate(total):
            sums[s][i] = x

    def own_hits(t):
        hits = jnp.int32(0)
        for k in range(listed):
            away = near_ref[k, t] - (first_tile + t)
            hits = hits + 1 - jnp.minimum(away * away, 1)
        return jnp.full((8, TILE), hits, jnp.int32).astype(jnp.float32)

    def finish(t, s, carry):
        totals, selfs = carry
        own = first_tile + t
        own_span = pl.ds(pl.multiple_of(own * TILE, TILE), TILE)
        out_span = pl.ds(pl.multiple_of(t * TILE, TILE), TILE)
        sub = rows_of(TILE)
        quad = sub % 4
        mine = cols[8:16, own_span]
        fold = []
        for i in range(2):
            x = sums[s][i, 0:8] + sums[s][i, 8:16]
            fold.append(x[:, :TILE] + x[:, TILE:])
        en = sums[s][2, 0:8] + sums[s][2, 8:16]
        totals = totals + mine * jnp.where(sub < 4, en[:, :TILE], en[:, TILE:])
        selfs = selfs + own_hits(t) * (mine * mine)
        pull = jnp.where(sub < 4, fold[0] * mine[0:1], fold[1] * mine[4:5])
        pull = pull[0:4] + pull[4:8]
        force = cols[0:3, own_span] * pull[3:4] - pull[0:3]
        for c in range(3):
            force_ref[c, :, out_span] = force[c : c + 1]
        return totals, selfs

    def step(m, carry):
        for s in range(unroll):
            t = unroll * m + s
            before = (s - 1) % unroll
            carry = finish(jnp.maximum(t - 1, 0), before, carry)
            geometry(jnp.minimum(t + 1, row_tiles - 1), (s + 1) % unroll)
            blocks(t, s)
        return carry

    zero = jnp.zeros((8, TILE), jnp.float32)
    sums[unroll - 1][...] = jnp.zeros(sums[unroll - 1].shape, jnp.float32)
    geometry(0, 0)
    carry = lax.fori_loop(0, row_tiles // unroll, step, (zero, zero))
    first = cols[8:16, pl.ds(pl.multiple_of(first_tile * TILE, TILE), TILE)]
    totals, selfs = finish(row_tiles - 1, unroll - 1, carry)
    selfs = selfs - own_hits(0) * (first * first)
    soft = rounded(lax.rsqrt(jnp.full((8, TILE), DELTA_SOFT, jnp.float32)))
    sub = rows_of(TILE)
    share[...] = totals - jnp.where(sub < 4, selfs * soft, 0.0)

    outs = [
        pltpu.make_async_copy(src, dst, out_sem.at[i])
        for i, (src, dst) in enumerate(
            ((force_ref, force_out), (new_coords_ref, new_coords_out), (new_velocities_ref, new_velocities_out))
        )
    ]
    for c in swaps:
        c.wait_recv()
    up = accept_ref[replica]
    low = accept_ref[lower]

    def swapped(out, ref, got):
        for c in range(3):
            up_flag = jnp.full((1, width), up, jnp.int32) == 1
            low_flag = jnp.full((1, width), low, jnp.int32) == 1
            out[c] = jnp.where(up_flag, got[1, c], jnp.where(low_flag, got[0, c], ref[c]))

    swapped(new_coords_ref, coords_ref, lam_coords)
    far_e = [
        copy(share, far_share.at[step - 1], send_part.at[2, step - 1], recv_part.at[2, step - 1], partner(step))
        for step in range(1, parts)
    ]
    for c in far_e:
        c.start()
    outs[0].start()
    swapped(new_velocities_ref, velocities_ref, lam_velocities)
    outs[1].start()
    outs[2].start()
    for c in far_c + far_x + near_c[0] + near_c[1] + swaps:
        c.wait_send()
    for c in far_e:
        c.wait()
    both = share[...]
    if parts == 2:
        both = both + far_share[0]
    elif parts > 2:
        both = jnp.zeros_like(both)
        for p in range(parts):
            for step in range(parts):
                here = jnp.full((8, TILE), lax.rem(part + step, parts), jnp.int32) == p
                both = both + jnp.where(here, share[...] if step == 0 else far_share[step - 1], 0.0)
    lane1 = lax.broadcasted_iota(jnp.int32, (1, TILE), 1)
    line = jnp.zeros((1, TILE), jnp.float32)
    for h in range(3):
        value = jnp.sum(both[h : h + 1] + both[4 + h : 5 + h])
        line = jnp.where(lane1 == h, value * (0.5 / atoms), line)
    energy_ref[...] = line
    for c in outs:
        c.wait()


def handed_on(line_ref, *refs):
    half = (len(refs) - 1) // 2
    refs[half][...] = line_ref[:, 0:3]
    for src, dst in zip(refs[:half], refs[half + 1 :]):
        dst[...] = src[...]


def per_device(
    coords, velocities, coupling, charges, types, type_sigma, type_eps, near_tiles, accept
):
    parts, width = lax.axis_size("atom"), coords.shape[2]
    atoms = parts * width
    listed = near_tiles.shape[1]
    unroll = math.gcd(width // TILE, UNROLL)
    vmem = pl.BlockSpec(memory_space=pltpu.VMEM)
    whole = pl.BlockSpec(memory_space=pl.ANY)
    f32, bf16, far = jnp.float32, jnp.bfloat16, max(parts - 1, 1)
    dma = pltpu.SemaphoreType.DMA
    rows = jax.ShapeDtypeStruct((3, 1, width), f32)
    line, force, new_coords, new_velocities = pl.pallas_call(
        partial(tiles_kernel, parts, listed),
        out_shape=(jax.ShapeDtypeStruct((1, TILE), f32), rows, rows, rows),
        in_specs=[whole] * 9,
        out_specs=(vmem,) + (whole,) * 3,
        scratch_shapes=[
            pltpu.SMEM((listed, width // TILE), jnp.int32),
            pltpu.SMEM(type_sigma.shape, f32),
            pltpu.SMEM(type_eps.shape, f32),
            pltpu.SMEM(accept.shape, jnp.int32),
            pltpu.VMEM((1, atoms), f32),
            pltpu.VMEM((1, atoms), jnp.int32),
            pltpu.VMEM((3, 1, width), f32),
            pltpu.VMEM((3, 1, width), f32),
            pltpu.VMEM((1, 2, width), f32),
            pltpu.VMEM((3, 1, width), f32),
            pltpu.VMEM((3, 1, width), f32),
            pltpu.VMEM((3, 1, width), f32),
            dma((9,)),
            dma((3,)),
            pltpu.VMEM((16, atoms), f32),
            pltpu.VMEM((atoms // TILE, TILE, DEPTH), bf16),
            pltpu.VMEM((DEPTH, COLS * width), bf16),
            pltpu.VMEM((atoms // TILE, 16, TILE), bf16),
            pltpu.VMEM((atoms // TILE, 16, TILE), bf16),
            pltpu.VMEM((far, 3, 1, width), f32),
            pltpu.VMEM((far, 1, 2, width), f32),
            pltpu.VMEM((2, parts, 1, 2, width), f32),
            pltpu.VMEM((2, 3, 1, width), f32),
            pltpu.VMEM((2, 3, 1, width), f32),
            pltpu.VMEM((8, TILE), f32),
            pltpu.VMEM((far, 8, TILE), f32),
            dma((3, far)),
            dma((3, far)),
            dma((PIECES, far)),
            dma((PIECES, far)),
            dma((2, parts)),
            dma((2, parts)),
            dma((2, 2)),
            dma((2, 2)),
        ]
        + [pltpu.VMEM((listed, TILE, COLS * TILE), f32)] * unroll
        + [pltpu.VMEM((3, 16, 2 * TILE), f32)] * unroll,
        compiler_params=pltpu.CompilerParams(collective_id=0, has_side_effects=True),
        name="tiles",
    )(
        near_tiles.T,
        type_sigma,
        type_eps,
        accept,
        charges.reshape(1, atoms),
        types.reshape(1, atoms),
        coords.transpose(1, 0, 2),
        velocities.transpose(1, 0, 2),
        coupling,
    )
    energies, *results = pl.pallas_call(
        handed_on,
        out_shape=(jax.ShapeDtypeStruct((1, 3), f32), rows, rows, rows),
        in_specs=[vmem] * 4,
        out_specs=(vmem,) * 4,
        name="handed_on",
    )(line, force, new_coords, new_velocities)
    return (energies, *(x.transpose(1, 0, 2) for x in results))


def solution(mesh):
    split = P("lam", None, "atom")
    return jax.shard_map(
        per_device,
        mesh=mesh,
        in_specs=(split, split, split, P(), P(), P(), P(), P("atom", None), P()),
        out_specs=(P("lam", None), split, split, split),
        check_vma=False,
    )
```
